32 devices in a mesh: fsdp: 32 (over z, y, x, core).
Axes of the slice: x: 2, y: 2, z: 4, core: 2. Of those that a mesh axis runs over, the one named last changes fastest.
Arguments:
- tokens: bfloat16 [8192, 2048], P('fsdp'), may hold values from -6 to 6
- attention_gain: bfloat16 [2048], replicated, may hold values from 0.099609375 to 1.8984375
- feedforward_gain: bfloat16 [2048], replicated, may hold values from 0.099609375 to 1.8984375
- joined_projection: bfloat16 [4096, 2048], P('fsdp'), may hold values from -0.125 to 0.125
- output_projection: bfloat16 [2048, 2048], P('fsdp'), may hold values from -0.75 to 0.75
- gate_weight: bfloat16 [8192, 2048], P('fsdp'), may hold values from -0.125 to 0.125
- up_weight: bfloat16 [8192, 2048], P('fsdp'), may hold values from -0.125 to 0.125
- down_weight: bfloat16 [8192, 2048], P('fsdp'), may hold values from -0.0625 to 0.0625
- joined_adapter_input: bfloat16 [2048, 128], P('fsdp'), may hold values from -0.125 to 0.125
- joined_adapter_output: bfloat16 [4096, 128], P('fsdp'), may hold values from -1.5 to 1.5
- output_adapter_input: bfloat16 [2048, 128], P('fsdp'), may hold values from -0.75 to 0.75
- output_adapter_output: bfloat16 [2048, 128], P('fsdp'), may hold values from -1.5 to 1.5
- gate_adapter_input: bfloat16 [2048, 128], P('fsdp'), may hold values from -0.125 to 0.125
- gate_adapter_output: bfloat16 [8192, 128], P('fsdp'), may hold values from -1.5 to 1.5
- upward_adapter_input: bfloat16 [2048, 128], P('fsdp'), may hold values from -0.125 to 0.125
- upward_adapter_output: bfloat16 [8192, 128], P('fsdp'), may hold values from -1.5 to 1.5
- down_adapter_input: bfloat16 [8192, 128], P('fsdp'), may hold values from -0.0625 to 0.0625
- down_adapter_output: bfloat16 [2048, 128], P('fsdp'), may hold values from -1.5 to 1.5
- lengths: int32 [15], replicated, may hold values from 128 to 1024, as said below
- adapter_set: int32 [15], replicated, may hold values from 0 to 7
- cotangent: bfloat16 [8192, 2048], P('fsdp'), may hold values from -6 to 6
Outputs:
- layer_output: bfloat16 [8192, 2048], P('fsdp')
- grad_tokens: float32 [8192, 2048], P('fsdp')
- grad_joined_entry: float32 [2048, 128], P('fsdp')
- grad_joined_exit: float32 [4096, 128], P('fsdp')
- grad_output_entry: float32 [2048, 128], P('fsdp')
- grad_output_exit: float32 [2048, 128], P('fsdp')
- grad_gate_entry: float32 [2048, 128], P('fsdp')
- grad_gate_exit: float32 [8192, 128], P('fsdp')
- grad_up_entry: float32 [2048, 128], P('fsdp')
- grad_up_exit: float32 [8192, 128], P('fsdp')
- grad_down_entry: float32 [8192, 128], P('fsdp')
- grad_down_exit: float32 [2048, 128], P('fsdp')
The draws below stay inside these ranges and needn't reach their ends.
Inputs may be any that keep to these rules, and one draw needn't show every extreme that they name: `lengths`: the sequences lie end to end in stream order and fill all 8192 tokens; one sequence has exactly 1024 tokens and one exactly 128.
All inputs are finite; a program needn't handle non-finite values.
Results may differ from the reference program's by a relative error of at most 0.017.
Values may be sent and summed in bfloat16 or wider, within the bound.
A program may use at most 384 MiB of HBM per device.

```python
import math
import jax
import jax.numpy as jnp
from jax import lax

MODEL_WIDTH = 2048
HEADS = 16
KV_HEADS = 8
HEAD_WIDTH = 128
FEED_HIDDEN = 8192
SETS = 8
ADAPTER_RANK = 16
MAXLEN = 1024
MINLEN = 128
TOKENS = 8192
NSEQ = 15
JOINED_ROWS = 4096
ATTENTION_WIDTH = 2048
ADAPTER_COLUMNS = 128


def draw_lengths(key, part):
    pairs = (NSEQ - 1) // 2
    key_sizes = jax.random.fold_in(key, 11)
    key_order = jax.random.fold_in(key, 12)
    sizes = jax.random.randint(key_sizes, (pairs,), MINLEN, MAXLEN - MINLEN + 1).astype(jnp.int32)
    sizes = jnp.where(jnp.arange(pairs) == 0, MINLEN, sizes).astype(jnp.int32)
    whole = jnp.concatenate([sizes, MAXLEN - sizes, jnp.full((1,), MAXLEN, jnp.int32)]).astype(jnp.int32)
    scores = jax.random.randint(key_order, (NSEQ,), 0, 1000000).astype(jnp.int32) * NSEQ + jnp.arange(NSEQ).astype(jnp.int32)
    order = jnp.argsort(scores, stable=True)
    return whole[order].astype(jnp.int32)


def with_ends(values, stream_key, least, largest):
    longest = values.shape.index(max(values.shape))
    spots = []
    for shift in (0, 1):
        where = [jax.random.randint(jax.random.fold_in(stream_key, axis), (), 0, length) for axis, length in enumerate(values.shape)]
        where[longest] = (where[longest] + shift) % values.shape[longest]
        spots.append(tuple(where))
    return values.at[spots[0]].set(least).at[spots[1]].set(largest)


def steps_of(own_key, shape, pieces, smallest, high):
    level = 1.0
    for dim, blocks in pieces:
        heights = jax.random.uniform(jax.random.fold_in(jax.random.fold_in(own_key, 6), dim), (blocks,), jnp.float32, smallest / len(pieces), high / len(pieces))
        level = level * jnp.repeat(jnp.exp(heights), shape[dim] // blocks).reshape((-1,) + (1,) * (len(shape) - 1 - dim))
    return level


def gaussian(key, extent, width, reach, cuts=(), kind=jnp.bfloat16):
    level = steps_of(key, extent, cuts, -0.22, 0.18) if cuts else 1.0
    entries = jax.random.normal(key, extent, jnp.float32) * width * level
    return jnp.minimum(jnp.maximum(entries, -reach), reach).astype(kind)


def setup_inputs(seed: int = 0) -> dict:
    splits = jax.random.split(jax.random.key(seed), 22)
    return {
        "tokens": gaussian(splits[0], (TOKENS, MODEL_WIDTH), 1.0, 6.0, ((0, 32),)),
        "attention_gain": jnp.clip(1.0 + 0.18 * jax.random.normal(splits[1], (MODEL_WIDTH,), jnp.float32), 0.099609375, 1.8984375).astype(jnp.bfloat16),
        "feedforward_gain": jnp.clip(1.0 + 0.18 * jax.random.normal(splits[2], (MODEL_WIDTH,), jnp.float32), 0.099609375, 1.8984375).astype(jnp.bfloat16),
        "joined_projection": gaussian(splits[3], (JOINED_ROWS, MODEL_WIDTH), MODEL_WIDTH ** -0.5, 0.125, ((0, 32),)),
        "output_projection": gaussian(splits[4], (MODEL_WIDTH, ATTENTION_WIDTH), (HEAD_WIDTH // 2) ** -0.5, 0.75, ((0, 32),)),
        "gate_weight": gaussian(splits[5], (FEED_HIDDEN, MODEL_WIDTH), MODEL_WIDTH ** -0.5, 0.125, ((0, 32),)),
        "up_weight": gaussian(splits[6], (FEED_HIDDEN, MODEL_WIDTH), MODEL_WIDTH ** -0.5, 0.125, ((0, 32),)),
        "down_weight": gaussian(splits[7], (FEED_HIDDEN, MODEL_WIDTH), FEED_HIDDEN ** -0.5, 0.0625, ((0, 32),)),
        "joined_adapter_input": gaussian(splits[8], (MODEL_WIDTH, ADAPTER_COLUMNS), MODEL_WIDTH ** -0.5, 0.125, ((0, 32),)),
        "joined_adapter_output": gaussian(splits[9], (JOINED_ROWS, ADAPTER_COLUMNS), ADAPTER_RANK ** -0.5, 1.5, ((0, 32),)),
        "output_adapter_input": gaussian(splits[10], (ATTENTION_WIDTH, ADAPTER_COLUMNS), (HEAD_WIDTH // 2) ** -0.5, 0.75, ((0, 32),)),
        "output_adapter_output": gaussian(splits[11], (MODEL_WIDTH, ADAPTER_COLUMNS), ADAPTER_RANK ** -0.5, 1.5, ((0, 32),)),
        "gate_adapter_input": gaussian(splits[12], (MODEL_WIDTH, ADAPTER_COLUMNS), MODEL_WIDTH ** -0.5, 0.125, ((0, 32),)),
        "gate_adapter_output": gaussian(splits[13], (FEED_HIDDEN, ADAPTER_COLUMNS), ADAPTER_RANK ** -0.5, 1.5, ((0, 32),)),
        "upward_adapter_input": gaussian(splits[14], (MODEL_WIDTH, ADAPTER_COLUMNS), MODEL_WIDTH ** -0.5, 0.125, ((0, 32),)),
        "upward_adapter_output": gaussian(splits[15], (FEED_HIDDEN, ADAPTER_COLUMNS), ADAPTER_RANK ** -0.5, 1.5, ((0, 32),)),
        "down_adapter_input": gaussian(splits[16], (FEED_HIDDEN, ADAPTER_COLUMNS), FEED_HIDDEN ** -0.5, 0.0625, ((0, 32),)),
        "down_adapter_output": gaussian(splits[17], (MODEL_WIDTH, ADAPTER_COLUMNS), ADAPTER_RANK ** -0.5, 1.5, ((0, 32),)),
        "lengths": draw_lengths(jax.random.fold_in(splits[21], 71), 0),
        "adapter_set": with_ends(jax.random.randint(splits[19], (NSEQ,), 0, SETS), jax.random.fold_in(splits[19], 1), 0, SETS - 1).astype(jnp.int32),
        "cotangent": gaussian(splits[20], (TOKENS, MODEL_WIDTH), 1.0, 6.0, ((0, 32),)),
    }


EPSILON = 1e-05
ADAPTER_SCALE = 0.5
ROTARY_BASE = 1000000.0
MASKED = -1e+30
HIGHEST = lax.Precision.HIGHEST

@jax.custom_vjp
def low(v):
    return lax.optimization_barrier(v.astype(jnp.bfloat16)).astype(jnp.float32)

@jax.custom_vjp
def low_back(v):
    return v

def low_keep(v):
    return (low(v), None)

def low_pass(kept, grad):
    return (grad,)

def back_keep(v):
    return (v, None)

def back_low(kept, grad):
    return (low(grad),)
low.defvjp(low_keep, low_pass)
low_back.defvjp(back_keep, back_low)

def rounded_both(value):
    return low_back(low(value))

def project(left, right):
    return lax.dot_general(left, right, (((1,), (1,)), ((), ())), precision=HIGHEST, preferred_element_type=jnp.float32)

def product(left, right):
    return jnp.dot(left, right, precision=HIGHEST, preferred_element_type=jnp.float32)

def sequence_info(lengths, adapter_set, first, number):
    ends = jnp.cumsum(lengths).astype(jnp.int32)
    starts = (ends - lengths).astype(jnp.int32)
    index = (first + jnp.arange(number)).astype(jnp.int32)
    member = (index[:, None] >= starts[None, :]) & (index[:, None] < ends[None, :])
    labels = (jnp.arange(lengths.shape[0]) + 1).astype(jnp.int32)
    sequence = lax.optimization_barrier(jnp.sum(jnp.where(member, labels[None, :], 0), axis=1)).astype(jnp.int32) - 1
    begin = lax.optimization_barrier(jnp.sum(jnp.where(member, starts[None, :], 0), axis=1)).astype(jnp.int32)
    chosen = lax.optimization_barrier(jnp.sum(jnp.where(member, adapter_set[None, :], 0), axis=1)).astype(jnp.int32)
    return (sequence, (index - begin).astype(jnp.int32), chosen)

def rotary_tables(position):
    half = HEAD_WIDTH // 2
    inverse = jnp.exp(jnp.arange(half, dtype=jnp.float32) * (-2.0 * math.log(ROTARY_BASE) / HEAD_WIDTH))
    angles = position.astype(jnp.float32)[:, None] * inverse[None, :]
    return (jnp.cos(angles)[:, None, :], jnp.sin(angles)[:, None, :])

def rotate(values, cosine, sine):
    half = values.shape[-1] // 2
    first_half = values[..., :half]
    second_half = values[..., half:]
    return jnp.concatenate([first_half * cosine - second_half * sine, second_half * cosine + first_half * sine], axis=-1)

def rms_gain(values, gain):
    scale = lax.rsqrt(lax.optimization_barrier(jnp.mean(values * values, axis=-1, keepdims=True)) + EPSILON)
    return values * scale * gain

def attention(query, key, value, sequence):
    total = query.shape[0]
    block = min(512, total)
    reach_back = ((MAXLEN - 2) // block + 1) * block
    group = HEADS // KV_HEADS
    key_padded = jnp.concatenate([jnp.zeros((reach_back, KV_HEADS, HEAD_WIDTH), jnp.float32), key], axis=0)
    value_padded = jnp.concatenate([jnp.zeros((reach_back, KV_HEADS, HEAD_WIDTH), jnp.float32), value], axis=0)
    sequence_padded = jnp.concatenate([jnp.full((reach_back,), -1, jnp.int32), sequence], axis=0)
    scale = HEAD_WIDTH ** (-0.5)

    def one_block(start):
        query_rows = lax.dynamic_slice_in_dim(query, start, block, 0).reshape(block, KV_HEADS, group, HEAD_WIDTH)
        key_rows = lax.dynamic_slice_in_dim(key_padded, start, reach_back + block, 0)
        value_rows = lax.dynamic_slice_in_dim(value_padded, start, reach_back + block, 0)
        query_seq = lax.dynamic_slice_in_dim(sequence, start, block, 0)
        key_seq = lax.dynamic_slice_in_dim(sequence_padded, start, reach_back + block, 0)
        query_index = start + jnp.arange(block).astype(jnp.int32)
        key_index = start - reach_back + jnp.arange(reach_back + block).astype(jnp.int32)
        allowed = (query_seq[:, None] == key_seq[None, :]) & (key_index[None, :] <= query_index[:, None])
        scores = low_back(jnp.einsum('qhgd,khd->hgqk', query_rows, key_rows, precision=HIGHEST) * scale)
        scores = jnp.where(allowed[None, None], scores, MASKED)
        top = lax.optimization_barrier(jnp.max(scores, axis=-1, keepdims=True))
        weights = jnp.exp(scores - top)
        probs = low(weights / lax.optimization_barrier(jnp.sum(weights, axis=-1, keepdims=True)))
        result = jnp.einsum('hgqk,khd->qhgd', probs, value_rows, precision=HIGHEST)
        return result.reshape(block, HEADS * HEAD_WIDTH)
    starts = (jnp.arange(total // block) * block).astype(jnp.int32)
    return lax.map(jax.checkpoint(one_block), starts).reshape(total, HEADS * HEAD_WIDTH)

def reference(tokens, attention_gain, feedforward_gain, joined_projection, output_projection, gate_weight, up_weight, down_weight, joined_adapter_input, joined_adapter_output, output_adapter_input, output_adapter_output, gate_adapter_input, gate_adapter_output, upward_adapter_input, upward_adapter_output, down_adapter_input, down_adapter_output, lengths, adapter_set, cotangent):
    sequence, position, chosen = sequence_info(lengths, adapter_set, 0, TOKENS)
    column_set = (jnp.arange(SETS * ADAPTER_RANK) // ADAPTER_RANK).astype(jnp.int32)
    select = column_set[None, :] == chosen[:, None]
    cosine, sine = rotary_tables(position)
    gain_one = attention_gain.astype(jnp.float32)
    gain_two = feedforward_gain.astype(jnp.float32)
    joined_full = joined_projection.astype(jnp.float32)
    output_full = output_projection.astype(jnp.float32)
    gate_full = gate_weight.astype(jnp.float32)
    up_full = up_weight.astype(jnp.float32)
    down_full = down_weight.astype(jnp.float32)
    attend_width = HEADS * HEAD_WIDTH
    kv_width = KV_HEADS * HEAD_WIDTH
    rows_block = min(2048, TOKENS)
    blocks = TOKENS // rows_block

    def adapter_low(values, stack):
        return rounded_both(jnp.where(select, product(values, stack), 0.0))

    def forward(inputs, stacks):
        f_entry, f_exit, o_entry, o_exit, g_entry, g_exit, u_entry, u_exit, d_entry, d_exit = stacks
        normed_one = low(rms_gain(inputs, gain_one))
        joined_low = adapter_low(normed_one, f_entry)
        projected = low_back(project(normed_one, joined_full) + ADAPTER_SCALE * project(joined_low, f_exit))
        query = low(rotate(projected[:, :attend_width].reshape(TOKENS, HEADS, HEAD_WIDTH), cosine, sine))
        key = low(rotate(projected[:, attend_width:attend_width + kv_width].reshape(TOKENS, KV_HEADS, HEAD_WIDTH), cosine, sine))
        value = low(projected[:, attend_width + kv_width:].reshape(TOKENS, KV_HEADS, HEAD_WIDTH))
        attended = rounded_both(attention(query, key, value, sequence))
        output_low = adapter_low(attended, o_entry)
        branch = low_back(project(attended, output_full) + ADAPTER_SCALE * project(output_low, o_exit))
        hidden_one = inputs + branch
        normed_two = low(rms_gain(hidden_one, gain_two))
        gate_low = adapter_low(normed_two, g_entry)
        up_low = adapter_low(normed_two, u_entry)

        def feed_block(parts):
            normed_rows, gate_rows, up_rows, select_rows = parts
            gate = low_back(project(normed_rows, gate_full) + ADAPTER_SCALE * project(gate_rows, g_exit))
            upward = low_back(project(normed_rows, up_full) + ADAPTER_SCALE * project(up_rows, u_exit))
            hidden = low(gate * jax.nn.sigmoid(gate) * upward)
            down_low = rounded_both(jnp.where(select_rows, product(hidden, d_entry), 0.0))
            return product(hidden, down_full) + ADAPTER_SCALE * project(down_low, d_exit)
        mixed = lax.map(jax.checkpoint(feed_block), (normed_two.reshape(blocks, rows_block, MODEL_WIDTH), gate_low.reshape(blocks, rows_block, SETS * ADAPTER_RANK), up_low.reshape(blocks, rows_block, SETS * ADAPTER_RANK), select.reshape(blocks, rows_block, SETS * ADAPTER_RANK)))
        return hidden_one + mixed.reshape(TOKENS, MODEL_WIDTH)
    stacks = (joined_adapter_input.astype(jnp.float32), joined_adapter_output.astype(jnp.float32), output_adapter_input.astype(jnp.float32), output_adapter_output.astype(jnp.float32), gate_adapter_input.astype(jnp.float32), gate_adapter_output.astype(jnp.float32), upward_adapter_input.astype(jnp.float32), upward_adapter_output.astype(jnp.float32), down_adapter_input.astype(jnp.float32), down_adapter_output.astype(jnp.float32))
    result, pullback = jax.vjp(forward, tokens.astype(jnp.float32), stacks)
    grad_inputs, grad_stacks = pullback(cotangent.astype(jnp.float32))
    return (result.astype(jnp.bfloat16), grad_inputs, grad_stacks[0], grad_stacks[1], grad_stacks[2], grad_stacks[3], grad_stacks[4], grad_stacks[5], grad_stacks[6], grad_stacks[7], grad_stacks[8], grad_stacks[9])
```

```python
import functools
import math

import jax
import jax.numpy as jnp
from jax import lax
from jax.experimental import pallas as pl
from jax.experimental.pallas import tpu as pltpu
from jax.sharding import PartitionSpec as P

HEADS = 16
KV_HEADS = 8
HEAD_WIDTH = 128
ADAPTER_RANK = 16
REACH = 4

EPSILON = 1e-05
ADAPTER_SCALE = 0.5
ROTARY_BASE = 1000000.0
MASKED = -1e30
MESH = pl.DeviceIdType.MESH
AXIS = "fsdp"
VMEM_LIMIT = 60 * 1024 * 1024


def shifted(value, steps):
    count = lax.axis_size(AXIS)
    leading, last = (max(0, -steps), min(count, count - steps))
    return lax.ppermute(value, AXIS, [(source, source + steps) for source in range(leading, last)])


def swapped(value, bit):
    count = lax.axis_size(AXIS)
    return lax.ppermute(value, AXIS, [(source, source ^ bit) for source in range(count)])


def project(left, right):
    return lax.dot_general(
        left, right, (((1,), (1,)), ((), ())), preferred_element_type=jnp.float32
    )


def product(left, right):
    return jnp.dot(left, right, preferred_element_type=jnp.float32)


def contract_rows(left, right):
    return lax.dot_general(
        left, right, (((0,), (0,)), ((), ())), preferred_element_type=jnp.float32
    )


def sequence_info(lengths, adapter_set, index):
    ends = jnp.cumsum(lengths)
    starts = ends - lengths
    member = (index[:, None] >= starts[None, :]) & (index[:, None] < ends[None, :])
    labels = lax.iota(jnp.int32, lengths.shape[0]) + 1
    sequence = jnp.sum(jnp.where(member, labels[None, :], 0), axis=1) - 1
    begin = jnp.sum(jnp.where(member, starts[None, :], 0), axis=1)
    chosen = jnp.sum(jnp.where(member, adapter_set[None, :], 0), axis=1)
    return (sequence, index - begin, chosen)


def adapter_mask(chosen, columns):
    column_set = lax.broadcasted_iota(jnp.int32, (1, columns), 1) // ADAPTER_RANK
    return column_set == chosen[:, None]


def masked(values, select):
    return jnp.where(select, values, 0.0).astype(jnp.bfloat16)


def rotary_tables(position):
    half = HEAD_WIDTH // 2
    inverse = jnp.exp(lax.iota(jnp.float32, half) * (-2.0 * math.log(ROTARY_BASE) / HEAD_WIDTH))
    angles = position.astype(jnp.float32)[:, None] * inverse[None, :]
    cosine, sine = jnp.cos(angles), jnp.sin(angles)
    return (
        jnp.concatenate([cosine, cosine], axis=1),
        jnp.concatenate([-sine, sine], axis=1),
    )


def norm_forward(values, gain):
    scale = lax.rsqrt(jnp.mean(values * values, axis=-1, keepdims=True) + EPSILON)
    unit = values * scale
    return (unit * gain, unit, scale)


def norm_backward(grad, unit, scale, gain):
    weighted = grad * gain
    return scale * (weighted - unit * jnp.mean(weighted * unit, axis=-1, keepdims=True))


def partner_of(me, bit):
    return me + bit - 2 * bit * ((me // bit) % 2)


def peer_of(me, mask):
    bit = 1
    while bit <= mask:
        if mask & bit:
            me = partner_of(me, bit)
        bit *= 2
    return me


def enter(me, bits):
    barrier = pltpu.get_barrier_semaphore()
    for bit in bits:
        pl.semaphore_signal(
            barrier, inc=1, device_id=(partner_of(me, bit),), device_id_type=MESH
        )
    pl.semaphore_wait(barrier, len(bits))


def gather_kernel(parts, count, *refs):
    ins, outs = refs[:count], refs[count : 2 * count]
    send, recv, local = refs[2 * count :]
    me = lax.axis_index(AXIS)
    enter(me, sorted({bit for part in parts for bit in part[3]}))
    kept = []
    for a in range(count):
        rows = ins[a].shape[0]
        own = pltpu.make_async_copy(
            ins[a], outs[a].at[pl.ds(pl.multiple_of(me * rows, rows), rows)], local.at[a]
        )
        own.start()
        kept.append(own)

    def block(p, mask):
        a, first, number, _ = parts[p]
        rows = ins[a].shape[0]
        start = pl.multiple_of(peer_of(me, mask) * rows + first, 8)
        return outs[a].at[pl.ds(start, number)]

    def copy(p, mask, bit):
        a, first, number, _ = parts[p]
        source = ins[a].at[pl.ds(first, number)] if mask == 0 else block(p, mask)
        return pltpu.make_async_remote_copy(
            src_ref=source,
            dst_ref=block(p, mask),
            send_sem=send.at[p, mask + bit],
            recv_sem=recv.at[p, mask + bit],
            device_id=(partner_of(me, bit),),
            device_id_type=MESH,
        )

    def arrive(p, mask, bit):
        pltpu.make_async_remote_copy(
            src_ref=block(p, mask),
            dst_ref=block(p, mask),
            send_sem=send.at[p, mask],
            recv_sem=recv.at[p, mask],
            device_id=(partner_of(me, bit),),
            device_id_type=MESH,
        ).wait_recv()

    sends, arrivals = [], []
    for p, (_, _, _, order) in enumerate(parts):
        for level, bit in enumerate(order):
            first = copy(p, 0, bit)
            first.start()
            sends.append(first)
            held = [0]
            for earlier in order[:level]:
                held = held + [mask + earlier for mask in held]
            for place, mask in enumerate(held):
                arrivals.append(((level, place, p), p, mask + bit, bit, order[level + 1 :]))
    arrivals.sort(key=lambda entry: entry[0])
    for _, p, mask, bit, later in arrivals:
        arrive(p, mask, bit)
        for following in later:
            onward = copy(p, mask, following)
            onward.start()
            sends.append(onward)
    for sent in sends:
        sent.wait_send()
    for own in kept:
        own.wait()


def gather_rows(arrays, parts, members, collective_id):
    count = len(arrays)
    moved = sum(a.size * 2 for a in arrays) * (members - 1)
    return pl.pallas_call(
        functools.partial(gather_kernel, parts, count),
        out_shape=[
            jax.ShapeDtypeStruct((members * a.shape[0], a.shape[1]), a.dtype) for a in arrays
        ],
        in_specs=[pl.BlockSpec(memory_space=pl.ANY)] * count,
        out_specs=[pl.BlockSpec(memory_space=pl.ANY)] * count,
        scratch_shapes=[
            pltpu.SemaphoreType.DMA((len(parts), members)),
            pltpu.SemaphoreType.DMA((len(parts), members)),
            pltpu.SemaphoreType.DMA((count,)),
        ],
        compiler_params=pltpu.CompilerParams(
            collective_id=collective_id, has_side_effects=True
        ),
        cost_estimate=pl.CostEstimate(flops=0, bytes_accessed=moved * 2, transcendentals=0),
        name="gather_rows",
    )(*arrays)


def reduce_kernel(order, members, in_ref, out_ref, total, outgoing, incoming, send, recv):
    me = lax.axis_index(AXIS)
    rows = out_ref.shape[0]
    enter(me, sorted(order))
    for mask in range(members):
        start = pl.multiple_of(peer_of(me, mask) * rows, 8)
        total[mask] = in_ref[pl.ds(start, rows), :]
    live = list(range(members))
    for bit in order:
        leaving = [mask for mask in live if mask & bit]
        live = [mask for mask in live if not mask & bit]
        copies = []
        for mask in leaving:
            outgoing[mask] = total[mask].astype(jnp.bfloat16)
            copy = pltpu.make_async_remote_copy(
                src_ref=outgoing.at[mask],
                dst_ref=incoming.at[mask],
                send_sem=send.at[mask],
                recv_sem=recv.at[mask],
                device_id=(partner_of(me, bit),),
                device_id_type=MESH,
            )
            copy.start()
            copies.append((mask, copy))
        for mask, copy in copies:
            copy.wait_recv()
            total[mask - bit] = total[mask - bit] + incoming[mask].astype(jnp.float32)
        for mask, copy in copies:
            copy.wait_send()
    out_ref[...] = total[0]


def reduce_rows(value, order, members, collective_id):
    rows, columns = value.shape[0] // members, value.shape[1]
    return pl.pallas_call(
        functools.partial(reduce_kernel, order, members),
        out_shape=jax.ShapeDtypeStruct((rows, columns), jnp.float32),
        in_specs=[pl.BlockSpec(memory_space=pltpu.VMEM)],
        out_specs=pl.BlockSpec(memory_space=pltpu.VMEM),
        scratch_shapes=[
            pltpu.VMEM((members, rows, columns), jnp.float32),
            pltpu.VMEM((members, rows, columns), jnp.bfloat16),
            pltpu.VMEM((members, rows, columns), jnp.bfloat16),
            pltpu.SemaphoreType.DMA((members,)),
            pltpu.SemaphoreType.DMA((members,)),
        ],
        compiler_params=pltpu.CompilerParams(
            collective_id=collective_id, has_side_effects=True, vmem_limit_bytes=VMEM_LIMIT
        ),
        name="reduce_rows",
    )(value)


def joined_kernel(turned, x_ref, w_ref, cos_ref, sin_ref, query_ref, pair_ref):
    step = pl.program_id(0)
    values = project(x_ref[...], w_ref[...])
    cosine, sine = cos_ref[...], sin_ref[...]
    heads = values.shape[1] // HEAD_WIDTH
    turn = step < turned
    pieces = []
    for h in range(heads):
        head = values[:, h * HEAD_WIDTH : (h + 1) * HEAD_WIDTH]
        rotated = head * cosine + pltpu.roll(head, HEAD_WIDTH // 2, 1) * sine
        pieces.append(jnp.where(turn, rotated, head).astype(jnp.bfloat16))
    result = jnp.concatenate(pieces, axis=1)
    half = pl.num_programs(0) // 2

    @pl.when(step < half)
    def _():
        query_ref[...] = result

    @pl.when(step >= half)
    def _():
        pair_ref[...] = result


def joined_heads(x, weight, cosine, sine):
    number, depth = x.shape
    tile = 512
    steps = weight.shape[0] // tile
    half = steps // 2
    turned = (HEADS + KV_HEADS) * HEAD_WIDTH // tile
    wide = half * tile
    return pl.pallas_call(
        functools.partial(joined_kernel, turned),
        out_shape=[jax.ShapeDtypeStruct((number, wide), jnp.bfloat16)] * 2,
        grid=(steps,),
        in_specs=[
            pl.BlockSpec((number, depth), lambda j: (0, 0), pipeline_mode=pl.Buffered(1)),
            pl.BlockSpec((tile, depth), lambda j: (j, 0)),
            pl.BlockSpec((number, HEAD_WIDTH), lambda j: (0, 0)),
            pl.BlockSpec((number, HEAD_WIDTH), lambda j: (0, 0)),
        ],
        out_specs=[
            pl.BlockSpec((number, tile), lambda j: (0, jnp.minimum(j, half - 1))),
            pl.BlockSpec((number, tile), lambda j: (0, jnp.maximum(j - half, 0))),
        ],
        compiler_params=pltpu.CompilerParams(vmem_limit_bytes=VMEM_LIMIT),
        cost_estimate=pl.CostEstimate(
            flops=2 * number * depth * weight.shape[0],
            bytes_accessed=2 * weight.size + 4 * x.size,
            transcendentals=0,
        ),
        name="joined_heads",
    )(x, weight, cosine, sine)


def make_bias(first, query_seq, key_seq, bias_ref):
    number, keys = bias_ref.shape
    row = lax.broadcasted_iota(jnp.int32, (number, keys), 0) + (keys - number)
    column = lax.broadcasted_iota(jnp.int32, (number, keys), 1)
    allowed = (query_seq == key_seq) & (column <= row)
    bias_ref[...] = jnp.where(allowed, 0.0, MASKED)


def softmax_of(query, keys, bias):
    scale = HEAD_WIDTH ** (-0.5)
    scores = jnp.concatenate([project(query, key) for key in keys], axis=1) * scale + bias
    top = jnp.max(scores, axis=-1, keepdims=True)
    weights = jnp.exp(scores - top)
    return weights * (1.0 / jnp.sum(weights, axis=-1, keepdims=True))


def attend_kernel(blocks, *refs):
    q_ref = refs[0]
    k_refs = refs[1 : 1 + blocks]
    v_refs = refs[1 + blocks : 1 + 2 * blocks]
    qs_ref, ks_ref, out_ref, bias_ref = refs[1 + 2 * blocks :]

    @pl.when(pl.program_id(0) == 0)
    def _():
        make_bias(0, qs_ref[...], ks_ref[...], bias_ref)

    keys = [ref[...] for ref in k_refs]
    number = keys[0].shape[0]
    for g in range(HEADS // KV_HEADS):
        columns = slice(g * HEAD_WIDTH, (g + 1) * HEAD_WIDTH)
        probs = softmax_of(q_ref[:, columns], keys, bias_ref[...]).astype(jnp.bfloat16)
        result = product(probs[:, :number], v_refs[0][...])
        for b in range(1, blocks):
            result += product(probs[:, b * number : (b + 1) * number], v_refs[b][...])
        out_ref[:, columns] = result.astype(jnp.bfloat16)


def attend(query, pairs, query_seq, key_seq):
    number, blocks = query.shape[0], len(pairs)
    group = HEADS // KV_HEADS
    keys = blocks * number
    key_spec = pl.BlockSpec((number, HEAD_WIDTH), lambda j: (0, j))
    value_spec = pl.BlockSpec((number, HEAD_WIDTH), lambda j: (0, KV_HEADS + j))
    wide_spec = pl.BlockSpec((number, group * HEAD_WIDTH), lambda j: (0, j))
    return pl.pallas_call(
        functools.partial(attend_kernel, blocks),
        out_shape=jax.ShapeDtypeStruct(query.shape, jnp.bfloat16),
        grid=(KV_HEADS,),
        in_specs=[wide_spec]
        + [key_spec] * blocks
        + [value_spec] * blocks
        + [
            pl.BlockSpec((number, 1), lambda j: (0, 0)),
            pl.BlockSpec((1, keys), lambda j: (0, 0)),
        ],
        out_specs=wide_spec,
        scratch_shapes=[pltpu.VMEM((number, keys), jnp.float32)],
        compiler_params=pltpu.CompilerParams(vmem_limit_bytes=VMEM_LIMIT),
        cost_estimate=pl.CostEstimate(
            flops=4 * HEADS * number * keys * HEAD_WIDTH,
            bytes_accessed=4 * query.size + 2 * sum(p.size for p in pairs),
            transcendentals=HEADS * number * keys,
        ),
        name="attend",
    )(query, *pairs, *pairs, query_seq, key_seq)


def attend_back_kernel(blocks, *refs):
    q_ref, g_ref = refs[:2]
    k_refs = refs[2 : 2 + blocks]
    v_refs = refs[2 + blocks : 2 + 2 * blocks]
    qs_ref, ks_ref, cos_ref, sin_ref = refs[2 + 2 * blocks : 6 + 2 * blocks]
    dq_ref, own_ref, away_ref, bias_ref = refs[6 + 2 * blocks :]

    @pl.when(pl.program_id(0) == 0)
    def _():
        make_bias(0, qs_ref[...], ks_ref[...], bias_ref)

    scale = HEAD_WIDTH ** (-0.5)
    keys = [ref[...] for ref in k_refs]
    number = keys[0].shape[0]
    key_back = [None] * blocks
    value_back = [None] * blocks
    for g in range(HEADS // KV_HEADS):
        columns = slice(g * HEAD_WIDTH, (g + 1) * HEAD_WIDTH)
        query, grad = q_ref[:, columns], g_ref[:, columns]
        probs = softmax_of(query, keys, bias_ref[...])
        back = jnp.concatenate([project(grad, ref[...]) for ref in v_refs], axis=1)
        center = jnp.sum(back * probs, axis=-1, keepdims=True)
        score_back = (probs * (back - center)).astype(jnp.bfloat16)
        probs = probs.astype(jnp.bfloat16)
        total = None
        for b in range(blocks):
            rows = slice(b * number, (b + 1) * number)
            part = product(score_back[:, rows], keys[b])
            total = part if total is None else total + part
            to_key = contract_rows(score_back[:, rows], query)
            to_value = contract_rows(probs[:, rows], grad)
            key_back[b] = to_key if g == 0 else key_back[b] + to_key
            value_back[b] = to_value if g == 0 else value_back[b] + to_value
        total = total * scale
        turned = total * cos_ref[...] - pltpu.roll(total, HEAD_WIDTH // 2, 1) * sin_ref[...]
        dq_ref[:, columns] = turned.astype(jnp.bfloat16)
    for b in range(blocks - 1):
        away_ref[b, 0] = (key_back[b] * scale).astype(jnp.bfloat16)
        away_ref[b, 1] = value_back[b].astype(jnp.bfloat16)
    own_ref[0] = key_back[blocks - 1] * scale
    own_ref[1] = value_back[blocks - 1]


def attend_back(query, grad, pairs, query_seq, key_seq, cosine, sine):
    number, blocks = query.shape[0], len(pairs)
    group = HEADS // KV_HEADS
    keys = blocks * number
    wide = KV_HEADS * HEAD_WIDTH
    key_spec = pl.BlockSpec((number, HEAD_WIDTH), lambda j: (0, j))
    value_spec = pl.BlockSpec((number, HEAD_WIDTH), lambda j: (0, KV_HEADS + j))
    wide_spec = pl.BlockSpec((number, group * HEAD_WIDTH), lambda j: (0, j))
    fixed = pl.BlockSpec((number, HEAD_WIDTH), lambda j: (0, 0))
    return pl.pallas_call(
        functools.partial(attend_back_kernel, blocks),
        out_shape=[
            jax.ShapeDtypeStruct(query.shape, jnp.bfloat16),
            jax.ShapeDtypeStruct((2, number, wide), jnp.float32),
            jax.ShapeDtypeStruct((blocks - 1, 2, number, wide), jnp.bfloat16),
        ],
        grid=(KV_HEADS,),
        in_specs=[wide_spec, wide_spec]
        + [key_spec] * blocks
        + [value_spec] * blocks
        + [
            pl.BlockSpec((number, 1), lambda j: (0, 0)),
            pl.BlockSpec((1, keys), lambda j: (0, 0)),
            fixed,
            fixed,
        ],
        out_specs=[
            wide_spec,
            pl.BlockSpec((2, number, HEAD_WIDTH), lambda j: (0, 0, j)),
            pl.BlockSpec((blocks - 1, 2, number, HEAD_WIDTH), lambda j: (0, 0, 0, j)),
        ],
        scratch_shapes=[pltpu.VMEM((number, keys), jnp.float32)],
        compiler_params=pltpu.CompilerParams(vmem_limit_bytes=VMEM_LIMIT),
        cost_estimate=pl.CostEstimate(
            flops=10 * HEADS * number * keys * HEAD_WIDTH,
            bytes_accessed=6 * query.size + 8 * sum(p.size for p in pairs),
            transcendentals=HEADS * number * keys,
        ),
        name="attend_back",
    )(query, grad, *pairs, *pairs, query_seq, key_seq, cosine, sine)


def feed_kernel(
    width, tile, x_ref, c_ref, gl_ref, ul_ref, db_ref, w_ref,
    mixed_ref, back_ref, grads_ref, mixed_acc, back_acc, grad_acc,
):
    step, last = pl.program_id(0), pl.num_programs(0) - 1
    rows, columns = x_ref.shape[0], gl_ref.shape[1]
    hid = w_ref.shape[0] // 3
    wg, wu, wd = (w_ref.at[pl.ds(i * hid, hid)] for i in range(3))
    main, side = slice(0, width), slice(width, width + columns)

    @pl.when(step == 0)
    def _():
        mixed_acc[...] = jnp.zeros_like(mixed_acc)
        back_acc[...] = jnp.zeros_like(back_acc)

    grad_acc[...] = jnp.zeros_like(grad_acc)

    @pl.loop(0, rows // tile)
    def _(i):
        at = pl.ds(pl.multiple_of(i * tile, tile), tile)
        x, cot = x_ref[at, :], c_ref[at, :]
        gl, ul, db = gl_ref[at, :], ul_ref[at, :], db_ref[at, :]
        gate = project(x, wg[:, main]) + project(gl, wg[:, side])
        up = project(x, wu[:, main]) + project(ul, wu[:, side])
        back = project(cot, wd[:, main]) + project(db, wd[:, side])
        sigma = 1.0 / (1.0 + jnp.exp(-gate))
        active = gate * sigma
        hidden = (active * up).astype(jnp.bfloat16)
        gate_back = (back * up * sigma * (1.0 + gate * (1.0 - sigma))).astype(jnp.bfloat16)
        up_back = (back * active).astype(jnp.bfloat16)
        mixed_acc[at, :] += product(hidden, wd[...])
        back_acc[at, main] += product(gate_back, wg[:, main]) + product(up_back, wu[:, main])
        back_acc[at, side] += product(gate_back, wg[:, side])
        back_acc[at, width + columns : width + 2 * columns] += product(up_back, wu[:, side])
        grad_acc[:, :columns] += contract_rows(gate_back, gl)
        grad_acc[:, columns : 2 * columns] += contract_rows(up_back, ul)
        grad_acc[:, 2 * columns :] += contract_rows(hidden, db)

    grads_ref[...] = grad_acc[...].astype(grads_ref.dtype)

    @pl.when(step == last)
    def _():
        mixed_ref[...] = mixed_acc[...].astype(mixed_ref.dtype)
        back_ref[...] = back_acc[...].astype(back_ref.dtype)


def feed(x, cot, gate_low, up_low, down_back, weights, shard):
    rows, width = x.shape
    columns = gate_low.shape[1]
    steps = weights.shape[0] // (3 * shard)
    tile = 256
    one = pl.Buffered(1)
    whole = lambda j: (0, 0)
    return pl.pallas_call(
        functools.partial(feed_kernel, width, tile),
        out_shape=[
            jax.ShapeDtypeStruct((rows, width + columns), jnp.bfloat16),
            jax.ShapeDtypeStruct((rows, width + 2 * columns), jnp.bfloat16),
            jax.ShapeDtypeStruct((steps * shard, 3 * columns), jnp.bfloat16),
        ],
        grid=(steps,),
        in_specs=[
            pl.BlockSpec((rows, width), whole, pipeline_mode=one),
            pl.BlockSpec((rows, width), whole, pipeline_mode=one),
            pl.BlockSpec((rows, columns), whole, pipeline_mode=one),
            pl.BlockSpec((rows, columns), whole, pipeline_mode=one),
            pl.BlockSpec((rows, columns), whole, pipeline_mode=one),
            pl.BlockSpec((3 * shard, width + columns), lambda j: (j, 0)),
        ],
        out_specs=[
            pl.BlockSpec((rows, width + columns), whole, pipeline_mode=one),
            pl.BlockSpec((rows, width + 2 * columns), whole, pipeline_mode=one),
            pl.BlockSpec((shard, 3 * columns), lambda j: (j, 0)),
        ],
        scratch_shapes=[
            pltpu.VMEM((rows, width + columns), jnp.float32),
            pltpu.VMEM((rows, width + 2 * columns), jnp.float32),
            pltpu.VMEM((shard, 3 * columns), jnp.float32),
        ],
        compiler_params=pltpu.CompilerParams(vmem_limit_bytes=VMEM_LIMIT),
        cost_estimate=pl.CostEstimate(
            flops=4 * rows * weights.size,
            bytes_accessed=2 * weights.size + 8 * x.size,
            transcendentals=rows * steps * shard,
        ),
        name="feed",
    )(x, cot, gate_low, up_low, down_back, weights)


def per_device(
    tokens,
    attention_gain,
    feedforward_gain,
    joined_projection,
    output_projection,
    gate_weight,
    up_weight,
    down_weight,
    joined_adapter_input,
    joined_adapter_output,
    output_adapter_input,
    output_adapter_output,
    gate_adapter_input,
    gate_adapter_output,
    upward_adapter_input,
    upward_adapter_output,
    down_adapter_input,
    down_adapter_output,
    lengths,
    adapter_set,
    cotangent,
):
    number, width = tokens.shape
    columns = joined_adapter_input.shape[1]
    devices = lax.axis_size(AXIS)
    kv_width = KV_HEADS * HEAD_WIDTH
    shard = gate_weight.shape[0]
    near, far = 1, devices // 4
    highest = devices // 2
    middle = [1 << i for i in range(1, devices.bit_length()) if (1 << i) < far]
    me = lax.axis_index(AXIS)
    first = me * number

    joined_shard = jnp.concatenate([joined_projection, joined_adapter_output], axis=1)
    output_shard = jnp.concatenate([output_projection, output_adapter_output], axis=1)
    entry_shard = jnp.concatenate(
        [output_adapter_input, gate_adapter_input, upward_adapter_input, down_adapter_output],
        axis=1,
    )
    feed_shard = jnp.concatenate(
        [
            jnp.concatenate([gate_weight, gate_adapter_output], axis=1),
            jnp.concatenate([up_weight, upward_adapter_output], axis=1),
            jnp.concatenate([down_weight, down_adapter_input], axis=1),
        ],
        axis=0,
    )
    up_order = tuple([highest, far] + middle + [near])
    down_order = tuple([highest, far] + middle[::-1] + [near])
    rows = joined_shard.shape[0]
    full_joined, full_f_entry = gather_rows(
        [joined_shard, joined_adapter_input],
        (
            (0, 0, rows // 2, up_order),
            (0, rows // 2, rows // 2, down_order),
            (1, 0, joined_adapter_input.shape[0], up_order),
        ),
        devices,
        1,
    )
    full_output = lax.all_gather(output_shard, AXIS, axis=0, tiled=True)
    full_entry = lax.all_gather(entry_shard, AXIS, axis=0, tiled=True)
    full_o_entry = full_entry[:, :columns]
    full_gu_entry = full_entry[:, columns : 3 * columns]
    full_d_exit = full_entry[:, 3 * columns :]
    groups, seen = [], set()
    for device in range(devices):
        if device not in seen:
            members = [device]
            for bit in middle + [highest]:
                members = members + [m ^ bit for m in members]
            groups.append(sorted(members))
            seen.update(members)
    full_feed = lax.all_gather(
        feed_shard, AXIS, axis=0, tiled=True, axis_index_groups=groups
    )

    offsets = lax.iota(jnp.int32, number)
    blocks = [me, me ^ near, me ^ far, me ^ far ^ near]
    index = jnp.concatenate([b * number + offsets for b in blocks])
    all_sequence, all_position, all_chosen = sequence_info(lengths, adapter_set, index)
    all_select = adapter_mask(all_chosen, columns)
    select = all_select[:number]
    cosine, sine = rotary_tables(all_position[:number])
    key_index = first - REACH * number + lax.iota(jnp.int32, (REACH + 1) * number)
    key_sequence, _, _ = sequence_info(lengths, adapter_set, key_index)
    query_seq = all_sequence[:number][:, None]
    key_seq = key_sequence[None, :]

    inputs = tokens.astype(jnp.float32)
    gain_one = attention_gain.astype(jnp.float32)
    gain_two = feedforward_gain.astype(jnp.float32)

    def group_rows(value):
        beside = swapped(value, near)
        across = swapped(value, far)
        return jnp.concatenate([value, beside, across, swapped(across, near)], axis=0)

    group_cot = group_rows(cotangent)

    normed_one, unit_one, scale_one = norm_forward(inputs, gain_one)
    normed_one = normed_one.astype(jnp.bfloat16)
    joined_low = masked(product(normed_one, full_f_entry), select)
    half_low = joined_low * ADAPTER_SCALE
    query, pair = joined_heads(
        jnp.concatenate([normed_one, half_low], axis=1), full_joined, cosine, sine
    )
    pairs = [shifted(pair, back) for back in range(REACH, 0, -1)] + [pair]
    attended = attend(query, pairs, query_seq, key_seq)
    output_low = masked(product(attended, full_o_entry), select)
    branch = project(
        jnp.concatenate([attended, output_low * ADAPTER_SCALE], axis=1), full_output
    )
    hidden_one = inputs + branch

    normed_two, unit_two, scale_two = norm_forward(hidden_one, gain_two)
    normed_two = normed_two.astype(jnp.bfloat16)
    group_normed = group_rows(normed_two)
    lows = masked(
        product(group_normed, full_gu_entry), jnp.concatenate([all_select, all_select], axis=1)
    )
    gate_low, up_low = lows[:, :columns], lows[:, columns:]
    down_back = masked(ADAPTER_SCALE * product(group_cot, full_d_exit), all_select)
    mixed_parts, back_parts, feed_grads = feed(
        group_normed,
        group_cot,
        gate_low * ADAPTER_SCALE,
        up_low * ADAPTER_SCALE,
        down_back,
        full_feed,
        shard,
    )

    def group_sum(parts):
        own, beside = parts[:number], parts[number : 2 * number]
        across, corner = parts[2 * number : 3 * number], parts[3 * number :]
        wide = jnp.float32
        far_sum = across.astype(wide) + swapped(corner, near).astype(wide)
        near_sum = own.astype(wide) + swapped(beside, near).astype(wide)
        return near_sum + swapped(far_sum.astype(jnp.bfloat16), far).astype(wide)

    back_sum = group_sum(back_parts)
    mixed_sum = group_sum(mixed_parts)
    low_back = masked(
        ADAPTER_SCALE * back_sum[:, width:], jnp.concatenate([select, select], axis=1)
    )
    normed_two_back = back_sum[:, :width] + project(low_back, full_gu_entry)
    hidden_back_one = cotangent.astype(jnp.float32) + norm_backward(
        normed_two_back, unit_two, scale_two, gain_two
    )
    branch_back = hidden_back_one.astype(jnp.bfloat16)

    down_low = masked(mixed_sum[:, width:], select)
    mixed = mixed_sum[:, :width] + ADAPTER_SCALE * project(down_low, full_d_exit)
    layer_output = (hidden_one + mixed).astype(jnp.bfloat16)

    through = product(branch_back, full_output)
    output_low_back = masked(ADAPTER_SCALE * through[:, width:], select)
    attended_back = (through[:, :width] + project(output_low_back, full_o_entry)).astype(
        jnp.bfloat16
    )
    query_back, own_back, away_back = attend_back(
        query, attended_back, pairs, query_seq, key_seq, cosine, sine
    )
    pair_back = own_back
    for back in range(REACH, 0, -1):
        pair_back = pair_back + shifted(away_back[REACH - back], -back).astype(jnp.float32)
    half = HEAD_WIDTH // 2
    key_back = pair_back[0].reshape(number, KV_HEADS, HEAD_WIDTH)
    rolled = jnp.concatenate([key_back[..., half:], key_back[..., :half]], axis=-1)
    key_back = key_back * cosine[:, None, :] - rolled * sine[:, None, :]
    joined_back = jnp.concatenate(
        [
            query_back,
            key_back.reshape(number, kv_width).astype(jnp.bfloat16),
            pair_back[1].astype(jnp.bfloat16),
        ],
        axis=1,
    )
    inward = product(joined_back, full_joined)
    joined_low_back = masked(ADAPTER_SCALE * inward[:, width:], select)
    normed_one_back = inward[:, :width] + project(joined_low_back, full_f_entry)
    grad_tokens = hidden_back_one + norm_backward(normed_one_back, unit_one, scale_one, gain_one)

    feed_rows = lax.psum_scatter(
        feed_grads, AXIS, scatter_dimension=0, tiled=True, axis_index_groups=groups
    ).astype(jnp.float32)
    early = jnp.concatenate(
        [
            contract_rows(attended, output_low_back),
            ADAPTER_SCALE * contract_rows(branch_back, output_low),
            contract_rows(normed_two, low_back),
            ADAPTER_SCALE * contract_rows(cotangent, down_low),
        ],
        axis=1,
    )
    late_exit = contract_rows(joined_back, half_low)
    late_entry = contract_rows(normed_one, joined_low_back)
    per_exit, per_entry = late_exit.shape[0] // devices, late_entry.shape[0] // devices
    late = jnp.concatenate(
        [
            late_exit.reshape(devices, per_exit, columns),
            late_entry.reshape(devices, per_entry, columns),
            early.reshape(devices, per_entry, 5, columns)
            .transpose(0, 2, 1, 3)
            .reshape(devices, 5 * per_entry, columns),
        ],
        axis=1,
    ).reshape(-1, columns)
    mine = reduce_rows(late, (near,) + tuple(middle) + (far, highest), devices, 2)

    def piece(at):
        return mine[per_exit + at * per_entry : per_exit + (at + 1) * per_entry]

    return (
        layer_output,
        grad_tokens,
        piece(0),
        mine[:per_exit],
        piece(1),
        piece(2),
        piece(3),
        feed_rows[:, :columns],
        piece(4),
        feed_rows[:, columns : 2 * columns],
        feed_rows[:, 2 * columns :],
        piece(5),
    )


def solution(mesh):
    split, copied = P(AXIS, None), P()
    placed = (split, copied, copied) + (split,) * 15 + (copied, copied, split)
    return jax.shard_map(
        per_device, mesh=mesh, in_specs=placed, out_specs=(split,) * 12, check_vma=False
    )
```

```python
import functools
import math

import jax
import jax.numpy as jnp
from jax import lax
from jax.experimental import pallas as pl
from jax.experimental.pallas import tpu as pltpu
from jax.sharding import PartitionSpec as P


HEADS = 16
KV_HEADS = 8
HEAD_WIDTH = 128
ADAPTER_RANK = 16
REACH = 4

EPSILON = 1e-05
ADAPTER_SCALE = 0.5
ROTARY_BASE = 1000000.0
MASKED = -1e30
MESH = pl.DeviceIdType.MESH
AXIS = "fsdp"
VMEM_LIMIT = 60 * 1024 * 1024


def swapped(value, bit):
    count = lax.axis_size(AXIS)
    return lax.ppermute(value, AXIS, [(source, source ^ bit) for source in range(count)])


def project(left, right):
    return lax.dot_general(
        left, right, (((1,), (1,)), ((), ())), preferred_element_type=jnp.float32
    )


def product(left, right):
    return jnp.dot(left, right, preferred_element_type=jnp.float32)


def contract_rows(left, right):
    return lax.dot_general(
        left, right, (((0,), (0,)), ((), ())), preferred_element_type=jnp.float32
    )


def sequence_info(lengths, adapter_set, index):
    ends = jnp.cumsum(lengths)
    starts = ends - lengths
    member = (index[:, None] >= starts[None, :]) & (index[:, None] < ends[None, :])
    labels = lax.iota(jnp.int32, lengths.shape[0]) + 1
    sequence = jnp.sum(jnp.where(member, labels[None, :], 0), axis=1) - 1
    begin = jnp.sum(jnp.where(member, starts[None, :], 0), axis=1)
    chosen = jnp.sum(jnp.where(member, adapter_set[None, :], 0), axis=1)
    return (sequence, index - begin, chosen)


def adapter_mask(chosen, columns):
    column_set = lax.broadcasted_iota(jnp.int32, (1, columns), 1) // ADAPTER_RANK
    return column_set == chosen[:, None]


def masked(values, select):
    return jnp.where(select, values, 0.0).astype(jnp.bfloat16)


def rotary_tables(position):
    half = HEAD_WIDTH // 2
    inverse = jnp.exp(lax.iota(jnp.float32, half) * (-2.0 * math.log(ROTARY_BASE) / HEAD_WIDTH))
    angles = position.astype(jnp.float32)[:, None] * inverse[None, :]
    cosine, sine = jnp.cos(angles), jnp.sin(angles)
    return (
        jnp.concatenate([cosine, cosine], axis=1),
        jnp.concatenate([-sine, sine], axis=1),
    )


def norm_forward(values, gain):
    scale = lax.rsqrt(jnp.mean(values * values, axis=-1, keepdims=True) + EPSILON)
    unit = values * scale
    return (unit * gain, unit, scale)


def norm_backward(grad, unit, scale, gain):
    weighted = grad * gain
    return scale * (weighted - unit * jnp.mean(weighted * unit, axis=-1, keepdims=True))


def partner_of(me, bit):
    return me + bit - 2 * bit * ((me // bit) % 2)


def peer_of(me, mask):
    bit = 1
    while bit <= mask:
        if mask & bit:
            me = partner_of(me, bit)
        bit *= 2
    return me


def enter(me, bits):
    barrier = pltpu.get_barrier_semaphore()
    for bit in bits:
        pl.semaphore_signal(
            barrier, inc=1, device_id=(partner_of(me, bit),), device_id_type=MESH
        )
    pl.semaphore_wait(barrier, len(bits))


def span(bits):
    held = [0]
    for bit in bits:
        held = held + [mask + bit for mask in held]
    return held


def gather_kernel(parts, slots, bits_moved, count, *refs):
    moved = len(bits_moved)
    ins, more = refs[:count], refs[count : count + (moved > 0)]
    outs = refs[count + len(more) : 2 * count + len(more)]
    away = refs[2 * count + len(more) : 2 * count + len(more) + moved]
    send, recv, local = refs[2 * count + len(more) + moved :]
    me = lax.axis_index(AXIS)
    enter(me, sorted({bit for part in parts for bit in part[3]}))

    def block(p, mask):
        a, first, number, _ = parts[p]
        rows = ins[a].shape[0]
        start = pl.multiple_of(peer_of(me, mask) % slots[a] * rows + first, 8)
        return outs[a].at[pl.ds(start, number)]

    def own(p):
        a, first, number, _ = parts[p]
        return ins[a].at[pl.ds(first, number)]

    def copy(p, mask, bit):
        return pltpu.make_async_remote_copy(
            src_ref=own(p) if mask == 0 else block(p, mask),
            dst_ref=block(p, mask),
            send_sem=send.at[p, mask + bit],
            recv_sem=recv.at[p, mask + bit],
            device_id=(partner_of(me, bit),),
            device_id_type=MESH,
        )

    def arrive(p, mask, bit):
        pltpu.make_async_remote_copy(
            src_ref=block(p, mask),
            dst_ref=block(p, mask),
            send_sem=send.at[p, mask],
            recv_sem=recv.at[p, mask],
            device_id=(partner_of(me, bit),),
            device_id_type=MESH,
        ).wait_recv()

    sends, arrivals = [], []
    for p, (_, _, _, order) in enumerate(parts):
        for level, bit in enumerate(order):
            first = copy(p, 0, bit)
            first.start()
            sends.append(first)
            for place, mask in enumerate(span(order[:level])):
                arrivals.append(((level, place, p), p, mask + bit, bit, order[level + 1 :]))
    kept = []
    for p in range(len(parts)):
        kept.append(pltpu.make_async_copy(own(p), block(p, 0), local.at[p]))
        kept[-1].start()
    arrivals.sort(key=lambda entry: entry[0])
    moves = [
        pltpu.make_async_remote_copy(
            src_ref=more[0],
            dst_ref=away[i],
            send_sem=send.at[len(parts), i],
            recv_sem=recv.at[len(parts), i],
            device_id=(partner_of(me, bit),),
            device_id_type=MESH,
        )
        for i, bit in enumerate(bits_moved)
    ]
    waiting = True
    for (level, _, _), p, mask, bit, later in arrivals:
        if waiting and level == 1:
            waiting = False
            for move in moves:
                move.start()
        arrive(p, mask, bit)
        for following in later:
            onward = copy(p, mask, following)
            onward.start()
            sends.append(onward)
    for move in moves:
        move.wait()
    for sent in sends:
        sent.wait_send()
    for copied in kept:
        copied.wait()


def gather_rows(arrays, parts, collective_id, slots, moved=None, bits_moved=()):
    count, devices = len(arrays), lax.axis_size(AXIS)
    shapes = [
        jax.ShapeDtypeStruct((times * a.shape[0], a.shape[1]), a.dtype)
        for a, times in zip(arrays, slots, strict=True)
    ]
    sent = 2 * sum(math.prod(shape.shape) for shape in shapes)
    if moved is not None:
        arrays = list(arrays) + [moved]
        shapes += [jax.ShapeDtypeStruct(moved.shape, moved.dtype)] * len(bits_moved)
    return pl.pallas_call(
        functools.partial(gather_kernel, parts, slots, bits_moved, count),
        out_shape=shapes,
        in_specs=[pl.BlockSpec(memory_space=pl.ANY)] * len(arrays),
        out_specs=[pl.BlockSpec(memory_space=pl.ANY)] * len(shapes),
        scratch_shapes=[
            pltpu.SemaphoreType.DMA((len(parts) + 1, devices)),
            pltpu.SemaphoreType.DMA((len(parts) + 1, devices)),
            pltpu.SemaphoreType.DMA((len(parts),)),
        ],
        compiler_params=pltpu.CompilerParams(
            collective_id=collective_id, has_side_effects=True
        ),
        cost_estimate=pl.CostEstimate(flops=0, bytes_accessed=8 * sent, transcendentals=0),
        name="gather_rows",
    )(*arrays)


class Halving:
    def __init__(self, me, parts, ins, outs, totals, outgoing, incoming, send, recv):
        self.me, self.parts, self.ins, self.outs = me, parts, ins, outs
        self.totals, self.outgoing, self.incoming = totals, outgoing, incoming
        self.send, self.recv = send, recv
        self.live = [sorted(span(part[4])) for part in parts]
        self.slots = [{mask: at for at, mask in enumerate(masks)} for masks in self.live]
        self.held = []
        for part, masks in zip(parts, self.live, strict=True):
            sent = part[4][0] if ins[part[5][0]].dtype == jnp.bfloat16 else 0
            kept = [mask for mask in masks if not mask & sent]
            self.held.append({mask: at for at, mask in enumerate(kept)})
        self.pending = [[] for _ in parts]
        self.every = []
        self.levels = max(len(part[4]) for part in parts)

    def given(self, p, mask):
        _, block, first, rows, _, places = self.parts[p]
        a, place = places
        if isinstance(place, int):
            start = pl.multiple_of(peer_of(self.me, mask) % place * block + first, 8)
        else:
            start = place[mask] * block + first
        return self.ins[a].at[pl.ds(start, rows)]

    def launch(self, p, level):
        bit = self.parts[p][4][level]
        leaving = [mask for mask in self.live[p] if mask & bit]
        self.live[p] = [mask for mask in self.live[p] if not mask & bit]
        for mask in leaving:
            at = self.slots[p][mask]
            source = self.given(p, mask) if level == 0 else None
            if source is None or source.dtype != jnp.bfloat16:
                place = self.held[p][mask]
                value = self.totals[p][place] if level else source[...]
                self.outgoing[p][place] = value.astype(jnp.bfloat16)
                source = self.outgoing[p].at[place]
            copy = pltpu.make_async_remote_copy(
                src_ref=source,
                dst_ref=self.incoming[p].at[at],
                send_sem=self.send.at[p, at],
                recv_sem=self.recv.at[p, at],
                device_id=(partner_of(self.me, bit),),
                device_id_type=MESH,
            )
            copy.start()
            self.pending[p].append((mask, bit, copy))
            self.every.append(copy)

    def begin(self):
        for p in range(len(self.parts)):
            self.launch(p, 0)

    def advance(self, level):
        for p in range(len(self.parts)):
            if level >= len(self.parts[p][4]):
                continue
            arrived, self.pending[p] = self.pending[p], []
            for mask, bit, copy in arrived:
                copy.wait_recv()
                onto, wide = self.held[p][mask - bit], jnp.float32
                if level:
                    held = self.totals[p][onto]
                else:
                    held = self.given(p, mask - bit)[...].astype(wide)
                came = self.incoming[p][self.slots[p][mask]].astype(wide)
                self.totals[p][onto] = held + came
            if level + 1 < len(self.parts[p][4]):
                self.launch(p, level + 1)

    def finish(self):
        for p, (a, _, first, rows, _, _) in enumerate(self.parts):
            self.outs[a][first : first + rows, :] = self.totals[p][0]
        for copy in self.every:
            copy.wait_send()


def reduce_kernel(parts, counts, *refs):
    inputs, outputs = counts
    number = len(parts)
    ins, outs = refs[:inputs], refs[inputs : inputs + outputs]
    rest = refs[inputs + outputs :]
    buffers = (rest[i * number : (i + 1) * number] for i in range(3))
    me = lax.axis_index(AXIS)
    enter(me, sorted({bit for part in parts for bit in part[4]}))
    halving = Halving(me, parts, ins, outs, *buffers, *rest[3 * number :])
    halving.begin()
    for level in range(halving.levels):
        halving.advance(level)
    halving.finish()


def reduce_plan(values, sums):
    parts, shapes, scratch = [], [], []
    for a, (places, orders) in enumerate(sums):
        members = 1 << len(orders[0])
        source = places[0]
        block = values[source].shape[0] // members
        columns = values[source].shape[1]
        shapes.append(jax.ShapeDtypeStruct((block, columns), jnp.float32))
        pieces = len(orders) if block % (16 * len(orders)) == 0 else 1
        rows = block // pieces
        for i in range(pieces):
            parts.append((a, block, i * rows, rows, orders[i], places))
            held = members // 2 if values[source].dtype == jnp.bfloat16 else members
            scratch.append(((held, rows, columns), (members, rows, columns)))
    most = max(shape[0] for _, shape in scratch)
    buffers = [pltpu.VMEM(shape, jnp.float32) for shape, _ in scratch]
    buffers += [pltpu.VMEM(shape, jnp.bfloat16) for shape, _ in scratch]
    buffers += [pltpu.VMEM(shape, jnp.bfloat16) for _, shape in scratch]
    buffers += [pltpu.SemaphoreType.DMA((len(parts), most))] * 2
    return tuple(parts), shapes, buffers


def reduce_rows(values, sums, collective_id):
    parts, shapes, buffers = reduce_plan(values, sums)
    sent = 2 * sum(value.size for value in values)
    return pl.pallas_call(
        functools.partial(reduce_kernel, parts, (len(values), len(sums))),
        out_shape=shapes,
        in_specs=[pl.BlockSpec(memory_space=pltpu.VMEM)] * len(values),
        out_specs=[pl.BlockSpec(memory_space=pltpu.VMEM)] * len(sums),
        scratch_shapes=buffers,
        compiler_params=pltpu.CompilerParams(
            collective_id=collective_id, has_side_effects=True, vmem_limit_bytes=VMEM_LIMIT
        ),
        cost_estimate=pl.CostEstimate(flops=0, bytes_accessed=16 * sent, transcendentals=0),
        name="reduce_rows",
    )(*values)


def greet(me, devices, steps, bits=(1,)):
    barrier = pltpu.get_barrier_semaphore()
    for bit in bits:
        pl.semaphore_signal(
            barrier, inc=1, device_id=(partner_of(me, bit),), device_id_type=MESH
        )
    for step in steps:
        for there in (me + step, me - step):
            pl.semaphore_signal(
                barrier, inc=1, device_id=((there + devices) % devices,), device_id_type=MESH
            )
    pl.semaphore_wait(barrier, len(bits) + 2 * len(steps))


def context_kernel(devices, pair_ref, out_ref, zero, send, recv, local):
    me = lax.axis_index(AXIS)
    greet(me, devices, (2, 4))
    even = me % 2 == 0
    partner = partner_of(me, 1)

    def copy(i, source, slot, there):
        return pltpu.make_async_remote_copy(
            src_ref=source,
            dst_ref=out_ref.at[slot],
            send_sem=send.at[i],
            recv_sem=recv.at[slot],
            device_id=(there,),
            device_id_type=MESH,
        )

    def arrive(slot):
        copy(0, out_ref.at[slot], slot, partner).wait_recv()

    two = copy(0, pair_ref, 2, (me + 2) % devices)
    four = copy(1, pair_ref, 0, (me + 4) % devices)
    own = copy(2, pair_ref, 3, partner)
    two_even = copy(3, out_ref.at[2], 1, partner)
    two_odd = copy(3, out_ref.at[2], 3, partner)
    four_odd = copy(2, out_ref.at[0], 1, partner)
    has_two, has_four = me >= 2, me >= 4

    @pl.when(me + 2 < devices)
    def _():
        two.start()

    @pl.when(me + 4 < devices)
    def _():
        four.start()

    @pl.when(even)
    def _():
        own.start()

    @pl.when(me < 4)
    def _():
        zero[...] = jnp.zeros_like(zero)
        pltpu.make_async_copy(zero, out_ref.at[0], local.at[0]).start()

    @pl.when(me < 2)
    def _():
        pltpu.make_async_copy(zero, out_ref.at[2], local.at[2]).start()

    lacks_three = me < 3
    lacks_one = me < 1

    @pl.when(lacks_three)
    def _():
        pltpu.make_async_copy(zero, out_ref.at[1], local.at[1]).start()

    @pl.when(lacks_one)
    def _():
        pltpu.make_async_copy(zero, out_ref.at[3], local.at[3]).start()

    @pl.when(has_two)
    def _():
        arrive(2)

    @pl.when(has_two & even)
    def _():
        two_even.start()

    @pl.when(has_two & (me % 2 == 1))
    def _():
        two_odd.start()

    @pl.when(has_four)
    def _():
        arrive(0)

    @pl.when(has_four & (me % 2 == 1))
    def _():
        four_odd.start()

    @pl.when(me >= 1)
    def _():
        arrive(3)

    @pl.when(me >= 3)
    def _():
        arrive(1)

    for lacks, slot in ((me < 4, 0), (me < 3, 1), (me < 2, 2), (me < 1, 3)):

        @pl.when(lacks)
        def _(slot=slot):
            pltpu.make_async_copy(zero, out_ref.at[slot], local.at[slot]).wait()

    @pl.when(me + 2 < devices)
    def _():
        two.wait_send()

    @pl.when(me + 4 < devices)
    def _():
        four.wait_send()

    @pl.when(even)
    def _():
        own.wait_send()

    @pl.when(has_two)
    def _():
        two_even.wait_send()

    @pl.when(has_four & (me % 2 == 1))
    def _():
        four_odd.wait_send()


def context_of(pair, collective_id):
    devices = lax.axis_size(AXIS)
    return pl.pallas_call(
        functools.partial(context_kernel, devices),
        out_shape=jax.ShapeDtypeStruct((REACH,) + pair.shape, pair.dtype),
        in_specs=[pl.BlockSpec(memory_space=pl.ANY)],
        out_specs=pl.BlockSpec(memory_space=pl.ANY),
        scratch_shapes=[
            pltpu.VMEM(pair.shape, pair.dtype),
            pltpu.SemaphoreType.DMA((REACH,)),
            pltpu.SemaphoreType.DMA((REACH,)),
            pltpu.SemaphoreType.DMA((REACH,)),
        ],
        compiler_params=pltpu.CompilerParams(
            collective_id=collective_id, has_side_effects=True, vmem_limit_bytes=VMEM_LIMIT
        ),
        cost_estimate=pl.CostEstimate(
            flops=0, bytes_accessed=64 * pair.size, transcendentals=0
        ),
        name="context",
    )(pair)


def context_back_kernel(devices, parts, away, own, mixed, *refs):
    out_ref, sum_ref, beside, going, coming, send, recv = refs[:7]
    number = len(parts)
    buffers = (refs[7 + i * number : 7 + (i + 1) * number] for i in range(3))
    me = lax.axis_index(AXIS)
    bits = sorted({bit for part in parts for bit in part[4]})
    greet(me, devices, (2, 4), bits)
    halving = Halving(me, parts, [mixed], [sum_ref], *buffers, *refs[7 + 3 * number :])
    even = me % 2 == 0
    partner = partner_of(me, 1)
    wide, narrow = jnp.float32, jnp.bfloat16

    def copy(i, h, source, target, there):
        return pltpu.make_async_remote_copy(
            src_ref=source,
            dst_ref=target,
            send_sem=send.at[h, i],
            recv_sem=recv.at[h, i],
            device_id=(there,),
            device_id_type=MESH,
        )

    shared = []
    for h in range(2):
        for i, slot in enumerate((3, 1)):
            shared.append(copy(i, h, away.at[slot, h], beside.at[i, h], partner))
            shared[-1].start()
    halving.begin()
    out_ref[...] = own[...]
    far = []
    for h in range(2):
        for i in range(2):
            shared[2 * h + i].wait_recv()
        one, three = beside[0, h].astype(wide), beside[1, h].astype(wide)
        going[0, h] = (away[2, h].astype(wide) + jnp.where(even, three, one)).astype(narrow)
        going[1, h] = (away[0, h].astype(wide) + jnp.where(even, 0.0, three)).astype(narrow)
        out_ref[h] += jnp.where(even, one, 0.0)
        for i, step in enumerate((2, 4)):
            move = copy(
                2 + i, h, going.at[i, h], coming.at[i, h], (me - step + devices) % devices
            )
            far.append((i, h, step, move))

            @pl.when(me >= step)
            def _(move=move):
                move.start()

    for level in range(halving.levels):
        halving.advance(level)
    for i, h, step, move in far:

        @pl.when(me + step < devices)
        def _(i=i, h=h, move=move):
            move.wait_recv()
            out_ref[h] += coming[i, h].astype(wide)

    halving.finish()
    for move in shared:
        move.wait_send()
    for i, h, step, move in far:

        @pl.when(me >= step)
        def _(move=move):
            move.wait_send()


def context_back(away, own, mixed, sums, collective_id):
    devices = lax.axis_size(AXIS)
    half = (2,) + own.shape
    parts, shapes, buffers = reduce_plan([mixed], sums)
    return pl.pallas_call(
        functools.partial(context_back_kernel, devices, parts),
        out_shape=[jax.ShapeDtypeStruct(own.shape, jnp.float32)] + shapes,
        in_specs=[pl.BlockSpec(memory_space=pltpu.VMEM)] * 3,
        out_specs=[pl.BlockSpec(memory_space=pltpu.VMEM)] * 2,
        scratch_shapes=[
            pltpu.VMEM(half, jnp.bfloat16),
            pltpu.VMEM(half, jnp.bfloat16),
            pltpu.VMEM(half, jnp.bfloat16),
            pltpu.SemaphoreType.DMA((2, 4)),
            pltpu.SemaphoreType.DMA((2, 4)),
        ]
        + buffers,
        compiler_params=pltpu.CompilerParams(
            collective_id=collective_id, has_side_effects=True, vmem_limit_bytes=VMEM_LIMIT
        ),
        cost_estimate=pl.CostEstimate(flops=0, bytes_accessed=64 * own.size, transcendentals=0),
        name="context_back",
    )(away, own, mixed)


def joined_kernel(turned, x_ref, w_ref, cos_ref, sin_ref, query_ref, pair_ref):
    step = pl.program_id(0)
    values = project(x_ref[...], w_ref[...])
    cosine, sine = cos_ref[...], sin_ref[...]
    heads = values.shape[1] // HEAD_WIDTH
    turn = step < turned
    pieces = []
    for h in range(heads):
        head = values[:, h * HEAD_WIDTH : (h + 1) * HEAD_WIDTH]
        rotated = head * cosine + pltpu.roll(head, HEAD_WIDTH // 2, 1) * sine
        pieces.append(jnp.where(turn, rotated, head).astype(jnp.bfloat16))
    result = jnp.concatenate(pieces, axis=1)
    half = pl.num_programs(0) // 2

    @pl.when(step < half)
    def _():
        query_ref[...] = result

    @pl.when(step >= half)
    def _():
        pair_ref[...] = result


def joined_heads(x, weight, cosine, sine):
    number, depth = x.shape
    tile = 512
    steps = weight.shape[0] // tile
    half = steps // 2
    turned = (HEADS + KV_HEADS) * HEAD_WIDTH // tile
    wide = half * tile
    return pl.pallas_call(
        functools.partial(joined_kernel, turned),
        out_shape=[jax.ShapeDtypeStruct((number, wide), jnp.bfloat16)] * 2,
        grid=(steps,),
        in_specs=[
            pl.BlockSpec((number, depth), lambda j: (0, 0), pipeline_mode=pl.Buffered(1)),
            pl.BlockSpec((tile, depth), lambda j: (j, 0)),
            pl.BlockSpec((number, HEAD_WIDTH), lambda j: (0, 0)),
            pl.BlockSpec((number, HEAD_WIDTH), lambda j: (0, 0)),
        ],
        out_specs=[
            pl.BlockSpec((number, tile), lambda j: (0, jnp.minimum(j, half - 1))),
            pl.BlockSpec((number, tile), lambda j: (0, jnp.maximum(j - half, 0))),
        ],
        compiler_params=pltpu.CompilerParams(vmem_limit_bytes=VMEM_LIMIT),
        cost_estimate=pl.CostEstimate(
            flops=2 * number * depth * weight.shape[0],
            bytes_accessed=2 * weight.size + 4 * x.size,
            transcendentals=0,
        ),
        name="joined_heads",
    )(x, weight, cosine, sine)


def make_bias(query_seq, key_seq, bias_ref):
    number, keys = bias_ref.shape
    row = lax.broadcasted_iota(jnp.int32, (number, keys), 0) + (keys - number)
    column = lax.broadcasted_iota(jnp.int32, (number, keys), 1)
    allowed = (query_seq == key_seq) & (column <= row)
    bias_ref[...] = jnp.where(allowed, 0.0, MASKED)


def softmax_of(query, keys, bias):
    scale = HEAD_WIDTH ** (-0.5)
    scores = jnp.concatenate([project(query, key) for key in keys], axis=1) * scale + bias
    top = jnp.max(scores, axis=-1, keepdims=True)
    weights = jnp.exp(scores - top)
    return weights * (1.0 / jnp.sum(weights, axis=-1, keepdims=True))


def attend_kernel(blocks, *refs):
    q_ref = refs[0]
    k_refs = refs[1 : 1 + blocks]
    v_refs = refs[1 + blocks : 1 + 2 * blocks]
    qs_ref, ks_ref, out_ref, bias_ref = refs[1 + 2 * blocks :]

    @pl.when(pl.program_id(0) == 0)
    def _():
        make_bias(qs_ref[...], ks_ref[...], bias_ref)

    keys = [ref[...] for ref in k_refs]
    number = keys[0].shape[0]
    for g in range(HEADS // KV_HEADS):
        columns = slice(g * HEAD_WIDTH, (g + 1) * HEAD_WIDTH)
        probs = softmax_of(q_ref[:, columns], keys, bias_ref[...]).astype(jnp.bfloat16)
        result = product(probs[:, :number], v_refs[0][...])
        for b in range(1, blocks):
            result += product(probs[:, b * number : (b + 1) * number], v_refs[b][...])
        out_ref[:, columns] = result.astype(jnp.bfloat16)


def context_specs(number, blocks):
    def at(b, shift):
        if b == blocks - 1:
            return pl.BlockSpec((number, HEAD_WIDTH), lambda j: (0, shift + j))
        return pl.BlockSpec((None, number, HEAD_WIDTH), lambda j: (b, 0, shift + j))

    return [at(b, 0) for b in range(blocks)] + [at(b, KV_HEADS) for b in range(blocks)]


def attend(query, context, pair, query_seq, key_seq):
    number, blocks = query.shape[0], context.shape[0] + 1
    pairs = [context] * (blocks - 1) + [pair]
    group = HEADS // KV_HEADS
    keys = blocks * number
    wide_spec = pl.BlockSpec((number, group * HEAD_WIDTH), lambda j: (0, j))
    return pl.pallas_call(
        functools.partial(attend_kernel, blocks),
        out_shape=jax.ShapeDtypeStruct(query.shape, jnp.bfloat16),
        grid=(KV_HEADS,),
        in_specs=[wide_spec]
        + context_specs(number, blocks)
        + [
            pl.BlockSpec((number, 1), lambda j: (0, 0)),
            pl.BlockSpec((1, keys), lambda j: (0, 0)),
        ],
        out_specs=wide_spec,
        scratch_shapes=[pltpu.VMEM((number, keys), jnp.float32)],
        compiler_params=pltpu.CompilerParams(vmem_limit_bytes=VMEM_LIMIT),
        cost_estimate=pl.CostEstimate(
            flops=4 * HEADS * number * keys * HEAD_WIDTH,
            bytes_accessed=4 * query.size + 2 * blocks * pair.size,
            transcendentals=HEADS * number * keys,
        ),
        name="attend",
    )(query, *pairs, *pairs, query_seq, key_seq)


def attend_back_kernel(blocks, *refs):
    q_ref, g_ref = refs[:2]
    k_refs = refs[2 : 2 + blocks]
    v_refs = refs[2 + blocks : 2 + 2 * blocks]
    qs_ref, ks_ref, cos_ref, sin_ref = refs[2 + 2 * blocks : 6 + 2 * blocks]
    dq_ref, own_ref, away_ref, bias_ref = refs[6 + 2 * blocks :]

    @pl.when(pl.program_id(0) == 0)
    def _():
        make_bias(qs_ref[...], ks_ref[...], bias_ref)

    scale = HEAD_WIDTH ** (-0.5)
    keys = [ref[...] for ref in k_refs]
    number = keys[0].shape[0]
    key_back = [None] * blocks
    value_back = [None] * blocks
    for g in range(HEADS // KV_HEADS):
        columns = slice(g * HEAD_WIDTH, (g + 1) * HEAD_WIDTH)
        query, grad = q_ref[:, columns], g_ref[:, columns]
        probs = softmax_of(query, keys, bias_ref[...])
        back = jnp.concatenate([project(grad, ref[...]) for ref in v_refs], axis=1)
        center = jnp.sum(back * probs, axis=-1, keepdims=True)
        score_back = (probs * (back - center)).astype(jnp.bfloat16)
        probs = probs.astype(jnp.bfloat16)
        total = None
        for b in range(blocks):
            rows = slice(b * number, (b + 1) * number)
            part = product(score_back[:, rows], keys[b])
            total = part if total is None else total + part
            to_key = contract_rows(score_back[:, rows], query)
            to_value = contract_rows(probs[:, rows], grad)
            key_back[b] = to_key if g == 0 else key_back[b] + to_key
            value_back[b] = to_value if g == 0 else value_back[b] + to_value
        total = total * scale
        turned = total * cos_ref[...] - pltpu.roll(total, HEAD_WIDTH // 2, 1) * sin_ref[...]
        dq_ref[:, columns] = turned.astype(jnp.bfloat16)
    for b in range(blocks - 1):
        away_ref[b, 0] = (key_back[b] * scale).astype(jnp.bfloat16)
        away_ref[b, 1] = value_back[b].astype(jnp.bfloat16)
    own_ref[0] = key_back[blocks - 1] * scale
    own_ref[1] = value_back[blocks - 1]


def attend_back(query, grad, context, pair, query_seq, key_seq, cosine, sine):
    number, blocks = query.shape[0], context.shape[0] + 1
    pairs = [context] * (blocks - 1) + [pair]
    group = HEADS // KV_HEADS
    keys = blocks * number
    wide = KV_HEADS * HEAD_WIDTH
    wide_spec = pl.BlockSpec((number, group * HEAD_WIDTH), lambda j: (0, j))
    fixed = pl.BlockSpec((number, HEAD_WIDTH), lambda j: (0, 0))
    return pl.pallas_call(
        functools.partial(attend_back_kernel, blocks),
        out_shape=[
            jax.ShapeDtypeStruct(query.shape, jnp.bfloat16),
            jax.ShapeDtypeStruct((2, number, wide), jnp.float32),
            jax.ShapeDtypeStruct((blocks - 1, 2, number, wide), jnp.bfloat16),
        ],
        grid=(KV_HEADS,),
        in_specs=[wide_spec, wide_spec]
        + context_specs(number, blocks)
        + [
            pl.BlockSpec((number, 1), lambda j: (0, 0)),
            pl.BlockSpec((1, keys), lambda j: (0, 0)),
            fixed,
            fixed,
        ],
        out_specs=[
            wide_spec,
            pl.BlockSpec((2, number, HEAD_WIDTH), lambda j: (0, 0, j)),
            pl.BlockSpec((blocks - 1, 2, number, HEAD_WIDTH), lambda j: (0, 0, 0, j)),
        ],
        scratch_shapes=[pltpu.VMEM((number, keys), jnp.float32)],
        compiler_params=pltpu.CompilerParams(vmem_limit_bytes=VMEM_LIMIT),
        cost_estimate=pl.CostEstimate(
            flops=10 * HEADS * number * keys * HEAD_WIDTH,
            bytes_accessed=6 * query.size + 8 * blocks * pair.size,
            transcendentals=HEADS * number * keys,
        ),
        name="attend_back",
    )(query, grad, *pairs, *pairs, query_seq, key_seq, cosine, sine)


def feed_kernel(pieces, joint, *refs):
    x_ref, c_ref, gl_ref, ul_ref, db_ref = refs[:5]
    w_refs = refs[5 : 5 + pieces]
    mixed_ref, back_ref, grads_ref, weights, mixed_acc, back_acc, arrival = refs[5 + pieces :]
    step = pl.program_id(0)
    width, columns = x_ref.shape[1], gl_ref.shape[1]
    rounds, hid = weights.shape[0], weights.shape[1] // 3
    height = hid // joint
    main, side = slice(0, width), slice(width, width + columns)

    def load(i, at, place):
        return [
            pltpu.make_async_copy(
                w_refs[i].at[pl.ds(j * height, height)],
                weights.at[at, pl.ds(j * hid + place * height, height)],
                arrival.at[at, place, j],
            )
            for j in range(3)
        ]

    @pl.when(step == 0)
    def _():
        for i in range(pieces):
            for copy in load(i, i // joint, i % joint):
                copy.start()
        grads_ref[...] = jnp.zeros_like(grads_ref)

    mixed_acc[...] = jnp.zeros_like(mixed_acc)
    back_acc[...] = jnp.zeros_like(back_acc)

    @pl.loop(0, rounds)
    def _(i):
        @pl.when(step == 0)
        def _():
            for place in range(joint):
                for copy in load(0, i, place):
                    copy.wait()

        wg, wu, wd = (weights.at[i, pl.ds(j * hid, hid)] for j in range(3))
        x, gl, ul, db = x_ref[...], gl_ref[...], ul_ref[...], db_ref[...]
        gate = project(x, wg[:, main]) + project(gl, wg[:, side])
        up = project(x, wu[:, main]) + project(ul, wu[:, side])
        back = project(c_ref[...], wd[:, main]) + project(db, wd[:, side])
        sigma = 1.0 / (1.0 + jnp.exp(-gate))
        active = gate * sigma
        hidden = (active * up).astype(jnp.bfloat16)
        gate_back = (back * up * sigma * (1.0 + gate * (1.0 - sigma))).astype(jnp.bfloat16)
        up_back = (back * active).astype(jnp.bfloat16)
        mixed_acc[...] += product(hidden, wd[...])
        back_acc[:, main] += product(gate_back, wg[:, main]) + product(up_back, wu[:, main])
        back_acc[:, side] += product(gate_back, wg[:, side])
        back_acc[:, width + columns :] += product(up_back, wu[:, side])
        at = pl.ds(pl.multiple_of(i * hid, hid), hid)
        grads_ref[at, :columns] += contract_rows(gate_back, gl)
        grads_ref[at, columns : 2 * columns] += contract_rows(up_back, ul)
        grads_ref[at, 2 * columns :] += contract_rows(hidden, db)

    mixed_ref[...] = mixed_acc[...].astype(jnp.bfloat16)
    back_ref[...] = back_acc[...].astype(jnp.bfloat16)


def feed(x, cot, gate_low, up_low, down_back, weights):
    (rows, width), columns = x.shape, gate_low.shape[1]
    pieces, height = len(weights), weights[0].shape[0] // 3
    hidden, tile = pieces * height, 256
    hid = min(512, hidden)
    row = lambda wide: pl.BlockSpec((tile, wide), lambda i: (i, 0))
    size = sum(w.size for w in weights)
    return pl.pallas_call(
        functools.partial(feed_kernel, pieces, hid // height),
        out_shape=[
            jax.ShapeDtypeStruct((rows, width + columns), jnp.bfloat16),
            jax.ShapeDtypeStruct((rows, width + 2 * columns), jnp.bfloat16),
            jax.ShapeDtypeStruct((hidden, 3 * columns), jnp.float32),
        ],
        grid=(rows // tile,),
        in_specs=[row(width)] * 2
        + [row(columns)] * 3
        + [pl.BlockSpec(memory_space=pl.ANY)] * pieces,
        out_specs=[
            row(width + columns),
            row(width + 2 * columns),
            pl.BlockSpec((hidden, 3 * columns), lambda i: (0, 0)),
        ],
        scratch_shapes=[
            pltpu.VMEM((hidden // hid, 3 * hid, width + columns), jnp.bfloat16),
            pltpu.VMEM((tile, width + columns), jnp.float32),
            pltpu.VMEM((tile, width + 2 * columns), jnp.float32),
            pltpu.SemaphoreType.DMA((hidden // hid, hid // height, 3)),
        ],
        compiler_params=pltpu.CompilerParams(vmem_limit_bytes=VMEM_LIMIT),
        cost_estimate=pl.CostEstimate(
            flops=4 * rows * size,
            bytes_accessed=2 * size + 14 * rows * width,
            transcendentals=rows * hidden,
        ),
        name="feed",
    )(x, cot, gate_low, up_low, down_back, *weights)


def layer(
    tokens,
    attention_gain,
    feedforward_gain,
    joined_projection,
    output_projection,
    gate_weight,
    up_weight,
    down_weight,
    joined_adapter_input,
    joined_adapter_output,
    output_adapter_input,
    output_adapter_output,
    gate_adapter_input,
    gate_adapter_output,
    upward_adapter_input,
    upward_adapter_output,
    down_adapter_input,
    down_adapter_output,
    lengths,
    adapter_set,
    cotangent,
):
    number, width = tokens.shape
    columns = joined_adapter_input.shape[1]
    devices = lax.axis_size(AXIS)
    kv_width = KV_HEADS * HEAD_WIDTH
    bits = [1 << i for i in range(devices.bit_length() - 1)]
    core, side, line = bits[:3]
    distant = bits[:2:-1]
    middle = bits[1:-2]
    me = lax.axis_index(AXIS)
    first = me * number

    joined_shard = jnp.concatenate([joined_projection, joined_adapter_output], axis=1)
    output_shard = jnp.concatenate([output_projection, output_adapter_output], axis=1)
    entry_shard = jnp.concatenate(
        [
            output_adapter_input,
            gate_adapter_input,
            upward_adapter_input,
            down_adapter_output,
            joined_adapter_input,
        ],
        axis=1,
    )
    half_shard = gate_weight.shape[0] // 2

    def feed_half(at):
        pairs = (
            (gate_weight, gate_adapter_output),
            (up_weight, upward_adapter_output),
            (down_weight, down_adapter_input),
        )
        cut = lambda value: value[at * half_shard : (at + 1) * half_shard]
        return jnp.concatenate(
            [jnp.concatenate([cut(left), cut(right)], axis=1) for left, right in pairs], axis=0
        )

    feed_first, feed_second = feed_half(0), feed_half(1)
    rows, output_rows, entry_rows = (
        value.shape[0] for value in (joined_shard, output_shard, entry_shard)
    )
    head = tuple(bits[:-3:-1])
    up_order, down_order = tuple(middle) + (core,), tuple(middle[::-1]) + (core,)
    full_joined, full_entry, full_output, *first_moved = gather_rows(
        [joined_shard, entry_shard, output_shard],
        (
            (0, 0, rows // 2, head + up_order),
            (0, rows // 2, rows // 2, head + down_order),
            (1, 0, entry_rows, head + up_order),
            (2, 0, output_rows // 2, head + down_order),
            (2, output_rows // 2, output_rows // 2, head + up_order),
        ),
        1,
        (devices,) * 3,
        feed_first,
        tuple(distant),
    )

    def spread(piece, moved):
        pieces = [piece]
        for bit, came in zip(distant, moved, strict=True):
            pieces.append(came)
            for held in pieces[1:-1]:
                pieces.append(swapped(held, bit))
        return pieces

    full_joined, *first_moved = lax.optimization_barrier((full_joined, *first_moved))
    first_pieces = spread(feed_first, first_moved)
    full_f_entry = full_entry[:, 4 * columns :]
    full_o_entry = full_entry[:, :columns]
    full_gu_entry = full_entry[:, columns : 3 * columns]
    full_d_exit = full_entry[:, 3 * columns : 4 * columns]

    members = 1 << 3
    place = me % members
    blocks = (me - place) * number
    index = blocks + lax.iota(jnp.int32, members * number)
    all_sequence, all_position, all_chosen = sequence_info(lengths, adapter_set, index)
    all_select = adapter_mask(all_chosen, columns)
    mine = lambda value: lax.dynamic_slice_in_dim(value, place * number, number, 0)
    select = mine(all_select)
    cosine, sine = rotary_tables(mine(all_position))
    key_index = first - REACH * number + lax.iota(jnp.int32, (REACH + 1) * number)
    key_sequence, _, _ = sequence_info(lengths, adapter_set, key_index)
    query_seq = mine(all_sequence)[:, None]
    key_seq = key_sequence[None, :]

    inputs = tokens.astype(jnp.float32)
    gain_one = attention_gain.astype(jnp.float32)
    gain_two = feedforward_gain.astype(jnp.float32)

    normed_one, unit_one, scale_one = norm_forward(inputs, gain_one)
    normed_one = normed_one.astype(jnp.bfloat16)
    joined_low = masked(product(normed_one, full_f_entry), select)
    half_low = joined_low * ADAPTER_SCALE
    query, pair = joined_heads(
        jnp.concatenate([normed_one, half_low], axis=1), full_joined, cosine, sine
    )
    context = context_of(pair, 4)
    context, feed_second = lax.optimization_barrier((context, feed_second))
    second_moved = []
    for bit in distant:
        second_moved.append(swapped(feed_second, bit))
    second_pieces = spread(feed_second, second_moved)
    attended = attend(query, context, pair, query_seq, key_seq)
    output_low = masked(product(attended, full_o_entry), select)
    branch = project(
        jnp.concatenate([attended, output_low * ADAPTER_SCALE], axis=1), full_output
    )
    hidden_one = inputs + branch

    normed_two, unit_two, scale_two = norm_forward(hidden_one, gain_two)
    normed_two = normed_two.astype(jnp.bfloat16)
    half_rows = number // 2
    up_group, down_group = (side, line, core), (line, side, core)
    group_normed, group_cot = gather_rows(
        [normed_two, cotangent],
        (
            (0, 0, half_rows, up_group),
            (0, half_rows, half_rows, down_group),
            (1, 0, half_rows, up_group),
            (1, half_rows, half_rows, down_group),
        ),
        5,
        (members, members),
    )
    both = jnp.concatenate([all_select, all_select], axis=1)
    lows = masked(product(group_normed, full_gu_entry), both) * ADAPTER_SCALE
    down_back = masked(ADAPTER_SCALE * product(group_cot, full_d_exit), all_select)
    mixed_parts, back_parts, feed_grads = feed(
        group_normed,
        group_cot,
        lows[:, :columns],
        lows[:, columns:],
        down_back,
        first_pieces + second_pieces,
    )
    up_sum, down_sum = (core, side, line), (core, line, side)
    (back_sum,) = reduce_rows([back_parts], [((0, members), (up_sum, down_sum) * 2)], 6)
    low_back = masked(
        ADAPTER_SCALE * back_sum[:, width:], jnp.concatenate([select, select], axis=1)
    )
    normed_two_back = back_sum[:, :width] + project(low_back, full_gu_entry)
    hidden_back_one = cotangent.astype(jnp.float32) + norm_backward(
        normed_two_back, unit_two, scale_two, gain_two
    )
    branch_back = hidden_back_one.astype(jnp.bfloat16)

    through = product(branch_back, full_output)
    output_low_back = masked(ADAPTER_SCALE * through[:, width:], select)
    attended_back = (through[:, :width] + project(output_low_back, full_o_entry)).astype(
        jnp.bfloat16
    )
    query_back, own_back, away = attend_back(
        query, attended_back, context, pair, query_seq, key_seq, cosine, sine
    )
    group_sums = ((0, members), (up_sum, down_sum))
    pair_back, mixed_sum = context_back(away, own_back, mixed_parts, [group_sums], 7)
    down_low = masked(mixed_sum[:, width:], select)
    mixed = mixed_sum[:, :width] + ADAPTER_SCALE * project(down_low, full_d_exit)
    layer_output = (hidden_one + mixed).astype(jnp.bfloat16)

    half = HEAD_WIDTH // 2
    key_back = pair_back[0].reshape(number, KV_HEADS, HEAD_WIDTH)
    rolled = jnp.concatenate([key_back[..., half:], key_back[..., :half]], axis=-1)
    key_back = key_back * cosine[:, None, :] - rolled * sine[:, None, :]
    joined_back = jnp.concatenate(
        [
            query_back,
            key_back.reshape(number, kv_width).astype(jnp.bfloat16),
            pair_back[1].astype(jnp.bfloat16),
        ],
        axis=1,
    )
    inward = product(joined_back, full_joined)
    joined_low_back = masked(ADAPTER_SCALE * inward[:, width:], select)
    normed_one_back = inward[:, :width] + project(joined_low_back, full_f_entry)
    grad_tokens = hidden_back_one + norm_backward(normed_one_back, unit_one, scale_one, gain_one)

    orders = ((core,) + tuple(middle) + head[::-1], (core,) + tuple(middle[::-1]) + head[::-1])
    low_grads = contract_rows(normed_two, low_back)
    totals = [
        contract_rows(attended, output_low_back),
        ADAPTER_SCALE * contract_rows(branch_back, output_low),
        low_grads[:, :columns],
        low_grads[:, columns:],
        ADAPTER_SCALE * contract_rows(cotangent, down_low),
        feed_grads,
        contract_rows(joined_back, half_low),
        contract_rows(normed_one, joined_low_back),
    ]
    sums = [((at, devices), orders) for at in range(len(totals))]
    blocks = len(first_pieces)
    feed_grads = feed_grads.reshape(2, blocks, half_shard, -1).transpose(1, 0, 2, 3)
    totals[5] = feed_grads.reshape(2 * blocks * half_shard, -1)
    sums[5] = ((5, {mask: at for at, mask in enumerate(span(distant))}), (tuple(distant[::-1]),))
    reduced = reduce_rows(totals, sums, 8)
    early, late = reduced[:6], (reduced[6], reduced[7])
    feed_rows = early[5]
    return (
        layer_output,
        grad_tokens,
        late[1],
        late[0],
        early[0],
        early[1],
        early[2],
        feed_rows[:, :columns],
        early[3],
        feed_rows[:, columns : 2 * columns],
        feed_rows[:, 2 * columns :],
        early[4],
    )


def solution(mesh):
    split, copied = P(AXIS, None), P()
    placed = (split, copied, copied) + (split,) * 15 + (copied, copied, split)
    return jax.shard_map(
        layer, mesh=mesh, in_specs=placed, out_specs=(split,) * 12, check_vma=False
    )
```

```python
import functools
import math

import jax
import jax.numpy as jnp
from jax import lax
from jax.experimental import pallas as pl
from jax.experimental.pallas import tpu as pltpu
from jax.sharding import PartitionSpec as P


HEADS = 16
KV_HEADS = 8
HEAD_WIDTH = 128
ADAPTER_RANK = 16
REACH = 4

EPSILON = 1e-05
ADAPTER_SCALE = 0.5
ROTARY_BASE = 1000000.0
MASKED = -1e30
MESH = pl.DeviceIdType.MESH
AXIS = "fsdp"
VMEM_LIMIT = 60 * 1024 * 1024


def swapped(value, bit):
    count = lax.axis_size(AXIS)
    return lax.ppermute(value, AXIS, [(source, source ^ bit) for source in range(count)])


def project(left, right):
    return lax.dot_general(
        left, right, (((1,), (1,)), ((), ())), preferred_element_type=jnp.float32
    )


def product(left, right):
    return jnp.dot(left, right, preferred_element_type=jnp.float32)


def contract_rows(left, right):
    return lax.dot_general(
        left, right, (((0,), (0,)), ((), ())), preferred_element_type=jnp.float32
    )


def sequence_info(lengths, adapter_set, index):
    ends = jnp.cumsum(lengths)
    starts = ends - lengths
    member = (index[:, None] >= starts[None, :]) & (index[:, None] < ends[None, :])
    labels = lax.iota(jnp.int32, lengths.shape[0]) + 1
    sequence = jnp.sum(jnp.where(member, labels[None, :], 0), axis=1) - 1
    begin = jnp.sum(jnp.where(member, starts[None, :], 0), axis=1)
    chosen = jnp.sum(jnp.where(member, adapter_set[None, :], 0), axis=1)
    return (sequence, index - begin, chosen)


def adapter_mask(chosen, columns):
    column_set = lax.broadcasted_iota(jnp.int32, (1, columns), 1) // ADAPTER_RANK
    return column_set == chosen[:, None]


def masked(values, select):
    return jnp.where(select, values, 0.0).astype(jnp.bfloat16)


def rotary_tables(position):
    half = HEAD_WIDTH // 2
    inverse = jnp.exp(lax.iota(jnp.float32, half) * (-2.0 * math.log(ROTARY_BASE) / HEAD_WIDTH))
    angles = position.astype(jnp.float32)[:, None] * inverse[None, :]
    cosine, sine = jnp.cos(angles), jnp.sin(angles)
    return (
        jnp.concatenate([cosine, cosine], axis=1),
        jnp.concatenate([-sine, sine], axis=1),
    )


def norm_forward(values, gain):
    scale = lax.rsqrt(jnp.mean(values * values, axis=-1, keepdims=True) + EPSILON)
    unit = values * scale
    return (unit * gain, unit, scale)


def norm_backward(grad, unit, scale, gain):
    weighted = grad * gain
    return scale * (weighted - unit * jnp.mean(weighted * unit, axis=-1, keepdims=True))


def partner_of(me, bit):
    return me + bit - 2 * bit * ((me // bit) % 2)


def peer_of(me, mask):
    bit = 1
    while bit <= mask:
        if mask & bit:
            me = partner_of(me, bit)
        bit *= 2
    return me


def enter(me, bits):
    barrier = pltpu.get_barrier_semaphore()
    for bit in bits:
        pl.semaphore_signal(
            barrier, inc=1, device_id=(partner_of(me, bit),), device_id_type=MESH
        )
    pl.semaphore_wait(barrier, len(bits))


def span(bits):
    held = [0]
    for bit in bits:
        held = held + [mask + bit for mask in held]
    return held


def gather_kernel(parts, slots, bits_moved, shared, count, *refs):
    extra = len(shared) or (len(bits_moved) > 0)
    added = 1 if shared else len(bits_moved)
    ins, more = refs[:count], refs[count : count + extra]
    outs = refs[count + extra : 2 * count + extra]
    away = refs[2 * count + extra : 2 * count + extra + added]
    send, recv, local, *stage = refs[2 * count + extra + added :]
    me = lax.axis_index(AXIS)
    enter(me, sorted({bit for part in parts for bit in part[3]}))

    def block(p, mask):
        a, first, number, _ = parts[p]
        rows = ins[a].shape[0]
        start = pl.multiple_of(peer_of(me, mask) % slots[a] * rows + first, 8)
        return outs[a].at[pl.ds(start, number)]

    def own(p):
        a, first, number, _ = parts[p]
        return ins[a].at[pl.ds(first, number)]

    def copy(p, mask, bit):
        return pltpu.make_async_remote_copy(
            src_ref=own(p) if mask == 0 else block(p, mask),
            dst_ref=block(p, mask),
            send_sem=send.at[p, mask + bit],
            recv_sem=recv.at[p, mask + bit],
            device_id=(partner_of(me, bit),),
            device_id_type=MESH,
        )

    def arrive(p, mask, bit):
        pltpu.make_async_remote_copy(
            src_ref=block(p, mask),
            dst_ref=block(p, mask),
            send_sem=send.at[p, mask],
            recv_sem=recv.at[p, mask],
            device_id=(partner_of(me, bit),),
            device_id_type=MESH,
        ).wait_recv()

    sends, arrivals = [], []
    for p, (_, _, _, order) in enumerate(parts):
        for level, bit in enumerate(order):
            first = copy(p, 0, bit)
            first.start()
            sends.append(first)
            for place, mask in enumerate(span(order[:level])):
                arrivals.append(((level, place, p), p, mask + bit, bit, order[level + 1 :]))
    kept, exchanged = [], []

    def keep(at, source, target):
        inward = pltpu.make_async_copy(source, stage[at], local.at[0, at])
        inward.start()
        kept.append((inward, pltpu.make_async_copy(stage[at], target, local.at[1, at])))

    def there(mask, first, rows):
        height = away[0].shape[0] // slots[-1]
        start = pl.multiple_of(peer_of(me, mask) % slots[-1] * height + first, 8)
        return away[0].at[pl.ds(start, rows)]

    def hand(at, source, target, bit):
        return pltpu.make_async_remote_copy(
            src_ref=source,
            dst_ref=target,
            send_sem=send.at[len(parts), at],
            recv_sem=recv.at[len(parts), at],
            device_id=(partner_of(me, bit),),
            device_id_type=MESH,
        )

    crossed = []
    for i, (mask, crossing) in enumerate(shared):
        if crossing is not None:
            first, rows, bit = crossing
            crossed.append(
                hand(8 + i, more[i].at[pl.ds(first, rows)], there(mask, first, rows), bit)
            )
            crossed[-1].start()
    for i, (mask, _) in enumerate(shared):
        rows = more[i].shape[0]
        exchanged.append(hand(i, more[i], there(mask, 0, rows), 1))
        exchanged[-1].start()
        keep(len(parts) + i, more[i], there(mask, 0, rows))
    for p in range(len(parts)):
        keep(p, own(p), block(p, 0))
    for inward, outward in kept:
        inward.wait()
        outward.start()
    arrivals.sort(key=lambda entry: entry[0])
    moves = [
        pltpu.make_async_remote_copy(
            src_ref=more[0],
            dst_ref=away[i],
            send_sem=send.at[len(parts), i],
            recv_sem=recv.at[len(parts), i],
            device_id=(partner_of(me, bit),),
            device_id_type=MESH,
        )
        for i, bit in enumerate(bits_moved)
    ]
    waiting = len(moves) > 0
    for (level, _, _), p, mask, bit, later in arrivals:
        if waiting and level == 1:
            waiting = False
            for move in moves:
                move.start()
        arrive(p, mask, bit)
        for following in later:
            onward = copy(p, mask, following)
            onward.start()
            sends.append(onward)
    crossings = [entry for entry in enumerate(shared) if entry[1][1] is not None]
    for (i, (mask, (first, rows, bit))), sent in zip(crossings, crossed, strict=True):
        came = there(mask + bit, first, rows)
        sent.wait_recv()
        exchanged.append(hand(16 + i, came, came, 1))
        exchanged[-1].start()
    for move in moves + exchanged:
        move.wait()
    for sent in crossed:
        sent.wait_send()
    for sent in sends:
        sent.wait_send()
    for _, outward in kept:
        outward.wait()


def gather_rows(arrays, parts, collective_id, slots, moved=None, bits_moved=(), shared=()):
    count, devices = len(arrays), lax.axis_size(AXIS)
    shapes = [
        jax.ShapeDtypeStruct((times * a.shape[0], a.shape[1]), a.dtype)
        for a, times in zip(arrays, slots)
    ]
    sent = 2 * sum(math.prod(shape.shape) for shape in shapes)
    if moved is not None:
        arrays = list(arrays) + [moved]
        shapes += [jax.ShapeDtypeStruct(moved.shape, moved.dtype)] * len(bits_moved)
    if shared:
        whole = shared[0][1]
        arrays = list(arrays) + [value for _, value, _ in shared]
        shape = (slots[-1] * whole.shape[0], whole.shape[1])
        shapes.append(jax.ShapeDtypeStruct(shape, whole.dtype))
    places = tuple((mask, crossing) for mask, _, crossing in shared)
    return pl.pallas_call(
        functools.partial(gather_kernel, parts, slots, bits_moved, places, count),
        out_shape=shapes,
        in_specs=[pl.BlockSpec(memory_space=pl.ANY)] * len(arrays),
        out_specs=[pl.BlockSpec(memory_space=pl.ANY)] * len(shapes),
        scratch_shapes=[
            pltpu.SemaphoreType.DMA((len(parts) + 1, devices)),
            pltpu.SemaphoreType.DMA((len(parts) + 1, devices)),
            pltpu.SemaphoreType.DMA((2, len(parts) + len(shared))),
        ]
        + [pltpu.VMEM((part[2], arrays[part[0]].shape[1]), arrays[part[0]].dtype) for part in parts]
        + [pltpu.VMEM(value.shape, value.dtype) for _, value, _ in shared],
        compiler_params=pltpu.CompilerParams(
            collective_id=collective_id, has_side_effects=True
        ),
        cost_estimate=pl.CostEstimate(flops=0, bytes_accessed=8 * sent, transcendentals=0),
        name="gather_rows",
    )(*arrays)


class Halving:
    def __init__(self, me, parts, ins, outs, totals, outgoing, incoming, send, recv):
        self.me, self.parts, self.ins, self.outs = me, parts, ins, outs
        self.totals, self.outgoing, self.incoming = totals, outgoing, incoming
        self.send, self.recv = send, recv
        self.pending = [[] for _ in parts]
        self.every = []
        self.levels = max(len(part[4]) for part in parts)

    def given(self, p, mask):
        _, block, first, rows, _, places = self.parts[p]
        a, place = places
        if isinstance(place, int):
            at = peer_of(self.me, mask) % place
        else:
            at = dict(place)[mask]
        return self.ins[a].at[pl.ds(pl.multiple_of(at * block + first, 8), rows)]

    def masks(self, p):
        return span(self.parts[p][4][:0:-1])

    def launch(self, p, level):
        order = self.parts[p][4]
        bit, half = order[level], 1 << (len(order) - 1 - level)
        copies = []
        if level:
            self.outgoing[p][half : 2 * half] = self.totals[p][half : 2 * half].astype(jnp.bfloat16)
            copies.append((self.outgoing[p].at[pl.ds(half, half)], half, half))
        else:
            for at, mask in enumerate(self.masks(p)):
                source = self.given(p, mask + bit)
                if source.dtype == jnp.bfloat16:
                    copies.append((source, half + at, None))
                else:
                    self.outgoing[p][half + at] = source[...].astype(jnp.bfloat16)
            if not copies:
                copies.append((self.outgoing[p].at[pl.ds(half, half)], half, half))
        for source, at, number in copies:
            there = at if number is None else pl.ds(at, number)
            copy = pltpu.make_async_remote_copy(
                src_ref=source,
                dst_ref=self.incoming[p].at[there],
                send_sem=self.send.at[p, at],
                recv_sem=self.recv.at[p, at],
                device_id=(partner_of(self.me, bit),),
                device_id_type=MESH,
            )
            copy.start()
            self.pending[p].append(copy)
            self.every.append(copy)

    def begin(self):
        for p in range(len(self.parts)):
            self.launch(p, 0)

    def advance(self, level):
        for p in range(len(self.parts)):
            order = self.parts[p][4]
            if level >= len(order):
                continue
            half, wide = 1 << (len(order) - 1 - level), jnp.float32
            arrived, self.pending[p] = self.pending[p], []
            for copy in arrived:
                copy.wait_recv()
            if level:
                came = self.incoming[p][half : 2 * half].astype(wide)
                self.totals[p][:half] = self.totals[p][:half] + came
            else:
                for at, mask in enumerate(self.masks(p)):
                    came = self.incoming[p][half + at].astype(wide)
                    self.totals[p][at] = self.given(p, mask)[...].astype(wide) + came
            if level + 1 < len(order):
                self.launch(p, level + 1)

    def finish(self):
        for p, (a, _, first, rows, _, _) in enumerate(self.parts):
            self.outs[a][first : first + rows, :] = self.totals[p][0]
        for copy in self.every:
            copy.wait_send()


def reduce_kernel(parts, counts, *refs):
    inputs, outputs = counts
    number = len(parts)
    ins, outs = refs[:inputs], refs[inputs : inputs + outputs]
    rest = refs[inputs + outputs :]
    buffers = (rest[i * number : (i + 1) * number] for i in range(3))
    me = lax.axis_index(AXIS)
    enter(me, sorted({bit for part in parts for bit in part[4]}))
    halving = Halving(me, parts, ins, outs, *buffers, *rest[3 * number :])
    halving.begin()
    for level in range(halving.levels):
        halving.advance(level)
    halving.finish()


def reduce_plan(values, sums):
    parts, shapes, scratch = [], [], []
    for a, (places, orders) in enumerate(sums):
        members = 1 << len(orders[0])
        source = places[0]
        block = values[source].shape[0] // members
        columns = values[source].shape[1]
        shapes.append(jax.ShapeDtypeStruct((block, columns), jnp.float32))
        pieces = len(orders) if block % (64 * len(orders)) == 0 else 1
        rows = block // pieces
        for i in range(pieces):
            parts.append((a, block, i * rows, rows, orders[(a + i) % len(orders)], places))
            out = members // 2 if values[source].dtype == jnp.bfloat16 else members
            scratch.append([(n, rows, columns) for n in (members // 2, out, members)])
    most = max(s[2][0] for s in scratch)
    kinds = (jnp.float32, jnp.bfloat16, jnp.bfloat16)
    buffers = [pltpu.VMEM(s[i], kinds[i]) for i in range(3) for s in scratch]
    buffers += [pltpu.SemaphoreType.DMA((len(parts), most))] * 2
    return tuple(parts), shapes, buffers


def reduce_rows(values, sums, collective_id):
    parts, shapes, buffers = reduce_plan(values, sums)
    sent = 2 * sum(value.size for value in values)
    return pl.pallas_call(
        functools.partial(reduce_kernel, parts, (len(values), len(sums))),
        out_shape=shapes,
        in_specs=[pl.BlockSpec(memory_space=pltpu.VMEM)] * len(values),
        out_specs=[pl.BlockSpec(memory_space=pltpu.VMEM)] * len(sums),
        scratch_shapes=buffers,
        compiler_params=pltpu.CompilerParams(
            collective_id=collective_id, has_side_effects=True, vmem_limit_bytes=VMEM_LIMIT
        ),
        cost_estimate=pl.CostEstimate(flops=0, bytes_accessed=16 * sent, transcendentals=0),
        name="reduce_rows",
    )(*values)


def greet(me, devices, steps, bits=(1,)):
    barrier = pltpu.get_barrier_semaphore()
    for bit in bits:
        pl.semaphore_signal(
            barrier, inc=1, device_id=(partner_of(me, bit),), device_id_type=MESH
        )
    for step in steps:
        for there in (me + step, me - step):
            pl.semaphore_signal(
                barrier, inc=1, device_id=((there + devices) % devices,), device_id_type=MESH
            )
    pl.semaphore_wait(barrier, len(bits) + 2 * len(steps))


def context_kernel(devices, pair_ref, out_ref, zero, send, recv, local):
    me = lax.axis_index(AXIS)
    greet(me, devices, (2, 4))
    even = me % 2 == 0
    partner = partner_of(me, 1)

    def copy(i, source, slot, there):
        return pltpu.make_async_remote_copy(
            src_ref=source,
            dst_ref=out_ref.at[slot],
            send_sem=send.at[i],
            recv_sem=recv.at[slot],
            device_id=(there,),
            device_id_type=MESH,
        )

    def arrive(slot):
        copy(0, out_ref.at[slot], slot, partner).wait_recv()

    two = copy(0, pair_ref, 2, (me + 2) % devices)
    four = copy(1, pair_ref, 0, (me + 4) % devices)
    own = copy(2, pair_ref, 3, partner)
    two_even = copy(3, out_ref.at[2], 1, partner)
    two_odd = copy(3, out_ref.at[2], 3, partner)
    four_odd = copy(2, out_ref.at[0], 1, partner)
    has_two, has_four = me >= 2, me >= 4

    @pl.when(me + 2 < devices)
    def _():
        two.start()

    @pl.when(me + 4 < devices)
    def _():
        four.start()

    @pl.when(even)
    def _():
        own.start()

    @pl.when(me < 4)
    def _():
        zero[...] = jnp.zeros_like(zero)
        pltpu.make_async_copy(zero, out_ref.at[0], local.at[0]).start()

    @pl.when(me < 2)
    def _():
        pltpu.make_async_copy(zero, out_ref.at[2], local.at[2]).start()

    lacks_three = me < 3
    lacks_one = me < 1

    @pl.when(lacks_three)
    def _():
        pltpu.make_async_copy(zero, out_ref.at[1], local.at[1]).start()

    @pl.when(lacks_one)
    def _():
        pltpu.make_async_copy(zero, out_ref.at[3], local.at[3]).start()

    @pl.when(has_two)
    def _():
        arrive(2)

    @pl.when(has_two & even)
    def _():
        two_even.start()

    @pl.when(has_two & (me % 2 == 1))
    def _():
        two_odd.start()

    @pl.when(has_four)
    def _():
        arrive(0)

    @pl.when(has_four & (me % 2 == 1))
    def _():
        four_odd.start()

    @pl.when(me >= 1)
    def _():
        arrive(3)

    @pl.when(me >= 3)
    def _():
        arrive(1)

    for lacks, slot in ((me < 4, 0), (me < 3, 1), (me < 2, 2), (me < 1, 3)):

        @pl.when(lacks)
        def _(slot=slot):
            pltpu.make_async_copy(zero, out_ref.at[slot], local.at[slot]).wait()

    @pl.when(me + 2 < devices)
    def _():
        two.wait_send()

    @pl.when(me + 4 < devices)
    def _():
        four.wait_send()

    @pl.when(even)
    def _():
        own.wait_send()

    @pl.when(has_two)
    def _():
        two_even.wait_send()

    @pl.when(has_four & (me % 2 == 1))
    def _():
        four_odd.wait_send()


def context_of(pair, collective_id):
    devices = lax.axis_size(AXIS)
    return pl.pallas_call(
        functools.partial(context_kernel, devices),
        out_shape=jax.ShapeDtypeStruct((REACH,) + pair.shape, pair.dtype),
        in_specs=[pl.BlockSpec(memory_space=pl.ANY)],
        out_specs=pl.BlockSpec(memory_space=pl.ANY),
        scratch_shapes=[
            pltpu.VMEM(pair.shape, pair.dtype),
            pltpu.SemaphoreType.DMA((REACH,)),
            pltpu.SemaphoreType.DMA((REACH,)),
            pltpu.SemaphoreType.DMA((REACH,)),
        ],
        compiler_params=pltpu.CompilerParams(
            collective_id=collective_id, has_side_effects=True, vmem_limit_bytes=VMEM_LIMIT
        ),
        cost_estimate=pl.CostEstimate(
            flops=0, bytes_accessed=64 * pair.size, transcendentals=0
        ),
        name="context",
    )(pair)


def context_back_kernel(devices, parts, counts, away, own, *refs):
    inputs, outputs = counts
    values, out_ref = refs[:inputs], refs[inputs]
    sums = refs[inputs + 1 : inputs + 1 + outputs]
    refs = refs[inputs + 1 + outputs :]
    beside, going, coming, send, recv = refs[:5]
    number = len(parts)
    buffers = (refs[5 + i * number : 5 + (i + 1) * number] for i in range(3))
    me = lax.axis_index(AXIS)
    bits = sorted({bit for part in parts for bit in part[4]})
    greet(me, devices, (2, 4), bits)
    halving = Halving(me, parts, values, sums, *buffers, *refs[5 + 3 * number :])
    even = me % 2 == 0
    partner = partner_of(me, 1)
    wide, narrow = jnp.float32, jnp.bfloat16

    def copy(i, c, source, target, there):
        return pltpu.make_async_remote_copy(
            src_ref=source,
            dst_ref=target,
            send_sem=send.at[c, i],
            recv_sem=recv.at[c, i],
            device_id=(there,),
            device_id_type=MESH,
        )

    pieces = own.shape[1] // 2
    chunks = [(h, pl.ds(r * pieces, pieces), 2 * h + r) for h in range(2) for r in range(2)]
    shared = []
    for h, rows, c in chunks:
        for i, slot in enumerate((3, 1)):
            shared.append(copy(i, c, away.at[slot, h, rows], beside.at[i, h, rows], partner))
            shared[-1].start()
    out_ref[...] = own[...]
    far = []
    for h, rows, c in chunks:
        for i in range(2):
            shared[2 * c + i].wait_recv()
        one, three = beside[0, h, rows].astype(wide), beside[1, h, rows].astype(wide)
        first = away[2, h, rows].astype(wide) + jnp.where(even, three, one)
        second = away[0, h, rows].astype(wide) + jnp.where(even, 0.0, three)
        going[0, h, rows] = first.astype(narrow)
        going[1, h, rows] = second.astype(narrow)
        out_ref[h, rows] += jnp.where(even, one, 0.0)
        for i, step in enumerate((2, 4)):
            move = copy(
                2 + i, c, going.at[i, h, rows], coming.at[i, h, rows],
                (me - step + devices) % devices,
            )
            far.append((i, h, rows, step, move))

            @pl.when(me >= step)
            def _(move=move):
                move.start()

    halving.begin()
    for level in range(halving.levels):
        halving.advance(level)
    for i, h, rows, step, move in far:

        @pl.when(me + step < devices)
        def _(i=i, h=h, rows=rows, move=move):
            move.wait_recv()
            out_ref[h, rows] += coming[i, h, rows].astype(wide)

    halving.finish()
    for move in shared:
        move.wait_send()
    for _, _, _, step, move in far:

        @pl.when(me >= step)
        def _(move=move):
            move.wait_send()


def context_back(away, own, values, sums, collective_id):
    devices = lax.axis_size(AXIS)
    half = (2,) + own.shape
    parts, shapes, buffers = reduce_plan(values, sums)
    in_vmem = pl.BlockSpec(memory_space=pltpu.VMEM)
    return pl.pallas_call(
        functools.partial(context_back_kernel, devices, parts, (len(values), len(sums))),
        out_shape=[jax.ShapeDtypeStruct(own.shape, jnp.float32)] + shapes,
        in_specs=[in_vmem] * (2 + len(values)),
        out_specs=[in_vmem] * (1 + len(sums)),
        scratch_shapes=[
            pltpu.VMEM(half, jnp.bfloat16),
            pltpu.VMEM(half, jnp.bfloat16),
            pltpu.VMEM(half, jnp.bfloat16),
            pltpu.SemaphoreType.DMA((4, 4)),
            pltpu.SemaphoreType.DMA((4, 4)),
        ]
        + buffers,
        compiler_params=pltpu.CompilerParams(
            collective_id=collective_id, has_side_effects=True, vmem_limit_bytes=67043328
        ),
        cost_estimate=pl.CostEstimate(flops=0, bytes_accessed=64 * own.size, transcendentals=0),
        name="context_back",
    )(away, own, *values)


def joined_kernel(turned, x_ref, w_ref, cos_ref, sin_ref, query_ref, pair_ref):
    step = pl.program_id(0)
    values = project(x_ref[...], w_ref[...])
    cosine, sine = cos_ref[...], sin_ref[...]
    heads = values.shape[1] // HEAD_WIDTH
    turn = step < turned
    pieces = []
    for h in range(heads):
        head = values[:, h * HEAD_WIDTH : (h + 1) * HEAD_WIDTH]
        rotated = head * cosine + pltpu.roll(head, HEAD_WIDTH // 2, 1) * sine
        pieces.append(jnp.where(turn, rotated, head).astype(jnp.bfloat16))
    result = jnp.concatenate(pieces, axis=1)
    half = pl.num_programs(0) // 2

    @pl.when(step < half)
    def _():
        query_ref[...] = result

    @pl.when(step >= half)
    def _():
        pair_ref[...] = result


def joined_heads(x, weight, cosine, sine):
    number, depth = x.shape
    tile = 512
    steps = weight.shape[0] // tile
    half = steps // 2
    turned = (HEADS + KV_HEADS) * HEAD_WIDTH // tile
    wide = half * tile
    return pl.pallas_call(
        functools.partial(joined_kernel, turned),
        out_shape=[jax.ShapeDtypeStruct((number, wide), jnp.bfloat16)] * 2,
        grid=(steps,),
        in_specs=[
            pl.BlockSpec((number, depth), lambda j: (0, 0), pipeline_mode=pl.Buffered(1)),
            pl.BlockSpec((tile, depth), lambda j: (j, 0)),
            pl.BlockSpec((number, HEAD_WIDTH), lambda j: (0, 0)),
            pl.BlockSpec((number, HEAD_WIDTH), lambda j: (0, 0)),
        ],
        out_specs=[
            pl.BlockSpec((number, tile), lambda j: (0, jnp.minimum(j, half - 1))),
            pl.BlockSpec((number, tile), lambda j: (0, jnp.maximum(j - half, 0))),
        ],
        compiler_params=pltpu.CompilerParams(vmem_limit_bytes=VMEM_LIMIT),
        cost_estimate=pl.CostEstimate(
            flops=2 * number * depth * weight.shape[0],
            bytes_accessed=2 * weight.size + 4 * x.size,
            transcendentals=0,
        ),
        name="joined_heads",
    )(x, weight, cosine, sine)


def make_bias(query_seq, key_seq, bias_ref):
    number, keys = bias_ref.shape
    row = lax.broadcasted_iota(jnp.int32, (number, keys), 0) + (keys - number)
    column = lax.broadcasted_iota(jnp.int32, (number, keys), 1)
    allowed = (query_seq == key_seq) & (column <= row)
    bias_ref[...] = jnp.where(allowed, 0.0, MASKED)


def softmax_of(query, keys, bias):
    scale = HEAD_WIDTH ** (-0.5)
    scores = jnp.concatenate([project(query, key) for key in keys], axis=1) * scale + bias
    top = jnp.max(scores, axis=-1, keepdims=True)
    weights = jnp.exp(scores - top)
    return weights * (1.0 / jnp.sum(weights, axis=-1, keepdims=True))


def attend_kernel(blocks, *refs):
    q_ref = refs[0]
    k_refs = refs[1 : 1 + blocks]
    v_refs = refs[1 + blocks : 1 + 2 * blocks]
    qs_ref, ks_ref, out_ref, bias_ref = refs[1 + 2 * blocks :]

    @pl.when(pl.program_id(0) == 0)
    def _():
        make_bias(qs_ref[...], ks_ref[...], bias_ref)

    keys = [ref[...] for ref in k_refs]
    number = keys[0].shape[0]
    for g in range(HEADS // KV_HEADS):
        columns = slice(g * HEAD_WIDTH, (g + 1) * HEAD_WIDTH)
        probs = softmax_of(q_ref[:, columns], keys, bias_ref[...]).astype(jnp.bfloat16)
        result = product(probs[:, :number], v_refs[0][...])
        for b in range(1, blocks):
            result += product(probs[:, b * number : (b + 1) * number], v_refs[b][...])
        out_ref[:, columns] = result.astype(jnp.bfloat16)


def context_specs(number, blocks):
    def at(b, shift):
        if b == blocks - 1:
            return pl.BlockSpec((number, HEAD_WIDTH), lambda j: (0, shift + j))
        return pl.BlockSpec((None, number, HEAD_WIDTH), lambda j: (b, 0, shift + j))

    return [at(b, 0) for b in range(blocks)] + [at(b, KV_HEADS) for b in range(blocks)]


def attend(query, context, pair, query_seq, key_seq):
    number, blocks = query.shape[0], context.shape[0] + 1
    pairs = [context] * (blocks - 1) + [pair]
    group = HEADS // KV_HEADS
    keys = blocks * number
    wide_spec = pl.BlockSpec((number, group * HEAD_WIDTH), lambda j: (0, j))
    return pl.pallas_call(
        functools.partial(attend_kernel, blocks),
        out_shape=jax.ShapeDtypeStruct(query.shape, jnp.bfloat16),
        grid=(KV_HEADS,),
        in_specs=[wide_spec]
        + context_specs(number, blocks)
        + [
            pl.BlockSpec((number, 1), lambda j: (0, 0)),
            pl.BlockSpec((1, keys), lambda j: (0, 0)),
        ],
        out_specs=wide_spec,
        scratch_shapes=[pltpu.VMEM((number, keys), jnp.float32)],
        compiler_params=pltpu.CompilerParams(vmem_limit_bytes=VMEM_LIMIT),
        cost_estimate=pl.CostEstimate(
            flops=4 * HEADS * number * keys * HEAD_WIDTH,
            bytes_accessed=4 * query.size + 2 * blocks * pair.size,
            transcendentals=HEADS * number * keys,
        ),
        name="attend",
    )(query, *pairs, *pairs, query_seq, key_seq)


def attend_back_kernel(blocks, *refs):
    q_ref, g_ref = refs[:2]
    k_refs = refs[2 : 2 + blocks]
    v_refs = refs[2 + blocks : 2 + 2 * blocks]
    qs_ref, ks_ref, cos_ref, sin_ref = refs[2 + 2 * blocks : 6 + 2 * blocks]
    dq_ref, own_ref, away_ref, bias_ref = refs[6 + 2 * blocks :]

    @pl.when(pl.program_id(0) == 0)
    def _():
        make_bias(qs_ref[...], ks_ref[...], bias_ref)

    scale = HEAD_WIDTH ** (-0.5)
    keys = [ref[...] for ref in k_refs]
    number = keys[0].shape[0]
    key_back = [None] * blocks
    value_back = [None] * blocks
    for g in range(HEADS // KV_HEADS):
        columns = slice(g * HEAD_WIDTH, (g + 1) * HEAD_WIDTH)
        query, grad = q_ref[:, columns], g_ref[:, columns]
        probs = softmax_of(query, keys, bias_ref[...])
        back = jnp.concatenate([project(grad, ref[...]) for ref in v_refs], axis=1)
        center = jnp.sum(back * probs, axis=-1, keepdims=True)
        score_back = (probs * (back - center)).astype(jnp.bfloat16)
        probs = probs.astype(jnp.bfloat16)
        total = None
        for b in range(blocks):
            rows = slice(b * number, (b + 1) * number)
            part = product(score_back[:, rows], keys[b])
            total = part if total is None else total + part
            to_key = contract_rows(score_back[:, rows], query)
            to_value = contract_rows(probs[:, rows], grad)
            key_back[b] = to_key if g == 0 else key_back[b] + to_key
            value_back[b] = to_value if g == 0 else value_back[b] + to_value
        total = total * scale
        turned = total * cos_ref[...] - pltpu.roll(total, HEAD_WIDTH // 2, 1) * sin_ref[...]
        dq_ref[:, columns] = turned.astype(jnp.bfloat16)
    for b in range(blocks - 1):
        away_ref[b, 0] = (key_back[b] * scale).astype(jnp.bfloat16)
        away_ref[b, 1] = value_back[b].astype(jnp.bfloat16)
    own_ref[0] = key_back[blocks - 1] * scale
    own_ref[1] = value_back[blocks - 1]


def attend_back(query, grad, context, pair, query_seq, key_seq, cosine, sine):
    number, blocks = query.shape[0], context.shape[0] + 1
    pairs = [context] * (blocks - 1) + [pair]
    group = HEADS // KV_HEADS
    keys = blocks * number
    wide = KV_HEADS * HEAD_WIDTH
    wide_spec = pl.BlockSpec((number, group * HEAD_WIDTH), lambda j: (0, j))
    fixed = pl.BlockSpec((number, HEAD_WIDTH), lambda j: (0, 0))
    return pl.pallas_call(
        functools.partial(attend_back_kernel, blocks),
        out_shape=[
            jax.ShapeDtypeStruct(query.shape, jnp.bfloat16),
            jax.ShapeDtypeStruct((2, number, wide), jnp.float32),
            jax.ShapeDtypeStruct((blocks - 1, 2, number, wide), jnp.bfloat16),
        ],
        grid=(KV_HEADS,),
        in_specs=[wide_spec, wide_spec]
        + context_specs(number, blocks)
        + [
            pl.BlockSpec((number, 1), lambda j: (0, 0)),
            pl.BlockSpec((1, keys), lambda j: (0, 0)),
            fixed,
            fixed,
        ],
        out_specs=[
            wide_spec,
            pl.BlockSpec((2, number, HEAD_WIDTH), lambda j: (0, 0, j)),
            pl.BlockSpec((blocks - 1, 2, number, HEAD_WIDTH), lambda j: (0, 0, 0, j)),
        ],
        scratch_shapes=[pltpu.VMEM((number, keys), jnp.float32)],
        compiler_params=pltpu.CompilerParams(vmem_limit_bytes=VMEM_LIMIT),
        cost_estimate=pl.CostEstimate(
            flops=10 * HEADS * number * keys * HEAD_WIDTH,
            bytes_accessed=6 * query.size + 8 * blocks * pair.size,
            transcendentals=HEADS * number * keys,
        ),
        name="attend_back",
    )(query, grad, *pairs, *pairs, query_seq, key_seq, cosine, sine)


def feed_kernel(pieces, joint, carried, *refs):
    x_ref, c_ref, gl_ref, ul_ref = refs[:4]
    w_refs, begun = refs[4 : 4 + pieces], refs[4 + pieces : 4 + pieces + carried]
    outs = refs[4 + pieces + carried :]
    mixed_ref, back_ref, grads_ref, weights, mixed_acc, back_acc, arrival = outs
    step = pl.program_id(0)
    width, columns = x_ref.shape[1], gl_ref.shape[1]
    rounds, hid = weights.shape[0], weights.shape[1] // 3
    height = hid // joint
    main, side = slice(0, width), slice(width, width + columns)

    def load(i, at, place):
        return [
            pltpu.make_async_copy(
                w_refs[i].at[pl.ds(j * height, height)],
                weights.at[at, pl.ds(j * hid + place * height, height)],
                arrival.at[at, place, j],
            )
            for j in range(3)
        ]

    @pl.when(step == 0)
    def _():
        for i in range(pieces):
            for copy in load(i, i // joint, i % joint):
                copy.start()
        grads_ref[...] = jnp.zeros_like(grads_ref)

    for acc, start in zip((mixed_acc, back_acc), begun or (None, None), strict=True):
        acc[...] = jnp.zeros_like(acc) if start is None else start[...].astype(jnp.float32)

    @pl.loop(0, rounds)
    def _(i):
        @pl.when(step == 0)
        def _():
            for place in range(joint):
                for copy in load(0, i, place):
                    copy.wait()

        wg, wu, wd = (weights.at[i, pl.ds(j * hid, hid)] for j in range(3))
        x, gl, ul = x_ref[...], gl_ref[...], ul_ref[...]
        gate = project(x, wg[:, main]) + project(gl, wg[:, side])
        up = project(x, wu[:, main]) + project(ul, wu[:, side])
        back = project(c_ref[...], wd[...])
        sigma = 1.0 / (1.0 + jnp.exp(-gate))
        active = gate * sigma
        hidden = (active * up).astype(jnp.bfloat16)
        gate_back = (back * up * sigma * (1.0 + gate * (1.0 - sigma))).astype(jnp.bfloat16)
        up_back = (back * active).astype(jnp.bfloat16)
        mixed_acc[...] += product(hidden, wd[...])
        back_acc[:, main] += product(gate_back, wg[:, main]) + product(up_back, wu[:, main])
        back_acc[:, side] += product(gate_back, wg[:, side])
        back_acc[:, width + columns :] += product(up_back, wu[:, side])
        at = pl.ds(pl.multiple_of(i * hid, hid), hid)
        grads_ref[at, :columns] += contract_rows(gate_back, gl)
        grads_ref[at, columns : 2 * columns] += contract_rows(up_back, ul)
        grads_ref[at, 2 * columns :] += contract_rows(hidden, c_ref[:, side])

    mixed_ref[...] = mixed_acc[...].astype(jnp.bfloat16)
    back_ref[...] = back_acc[...].astype(jnp.bfloat16)


def feed(x, cot, gate_low, up_low, weights, begun=()):
    (rows, width), columns = x.shape, gate_low.shape[1]
    pieces, height = len(weights), weights[0].shape[0] // 3
    hidden, tile = pieces * height, 256
    hid = min(512, hidden)
    row = lambda wide: pl.BlockSpec((tile, wide), lambda i: (i, 0))
    size = sum(w.size for w in weights)
    return pl.pallas_call(
        functools.partial(feed_kernel, pieces, hid // height, len(begun)),
        out_shape=[
            jax.ShapeDtypeStruct((rows, width + columns), jnp.bfloat16),
            jax.ShapeDtypeStruct((rows, width + 2 * columns), jnp.bfloat16),
            jax.ShapeDtypeStruct((hidden, 3 * columns), jnp.float32),
        ],
        grid=(rows // tile,),
        in_specs=[row(width), row(width + columns), row(columns), row(columns)]
        + [pl.BlockSpec(memory_space=pl.ANY)] * pieces
        + [row(value.shape[1]) for value in begun],
        out_specs=[
            row(width + columns),
            row(width + 2 * columns),
            pl.BlockSpec((hidden, 3 * columns), lambda i: (0, 0)),
        ],
        scratch_shapes=[
            pltpu.VMEM((hidden // hid, 3 * hid, width + columns), jnp.bfloat16),
            pltpu.VMEM((tile, width + columns), jnp.float32),
            pltpu.VMEM((tile, width + 2 * columns), jnp.float32),
            pltpu.SemaphoreType.DMA((hidden // hid, hid // height, 3)),
        ],
        compiler_params=pltpu.CompilerParams(vmem_limit_bytes=VMEM_LIMIT),
        cost_estimate=pl.CostEstimate(
            flops=4 * rows * size,
            bytes_accessed=2 * size + 14 * rows * width,
            transcendentals=rows * hidden,
        ),
        name="feed",
    )(x, cot, gate_low, up_low, *weights, *begun)


def layer(
    tokens,
    attention_gain,
    feedforward_gain,
    joined_projection,
    output_projection,
    gate_weight,
    up_weight,
    down_weight,
    joined_adapter_input,
    joined_adapter_output,
    output_adapter_input,
    output_adapter_output,
    gate_adapter_input,
    gate_adapter_output,
    upward_adapter_input,
    upward_adapter_output,
    down_adapter_input,
    down_adapter_output,
    lengths,
    adapter_set,
    cotangent,
):
    number, width = tokens.shape
    columns = joined_adapter_input.shape[1]
    devices = lax.axis_size(AXIS)
    kv_width = KV_HEADS * HEAD_WIDTH
    bits = [1 << i for i in range(devices.bit_length() - 1)]
    core, side, line = bits[:3]
    distant = bits[:2:-1]
    middle = bits[1:-2]
    me = lax.axis_index(AXIS)
    first = me * number

    joined_shard = jnp.concatenate([joined_projection, joined_adapter_output], axis=1)
    output_shard = jnp.concatenate([output_projection, output_adapter_output], axis=1)
    half_shard = gate_weight.shape[0] // 2

    def feed_half(at):
        pairs = (
            (gate_weight, gate_adapter_output),
            (up_weight, upward_adapter_output),
            (down_weight, down_adapter_input),
        )
        cut = lambda value: value[at * half_shard : (at + 1) * half_shard]
        return jnp.concatenate(
            [jnp.concatenate([cut(left), cut(right)], axis=1) for left, right in pairs], axis=0
        )

    feed_first, feed_second = feed_half(0), feed_half(1)
    entries = [
        joined_adapter_input,
        output_adapter_input,
        gate_adapter_input,
        upward_adapter_input,
        down_adapter_output,
    ]
    rows, output_rows, entry_rows = (
        value.shape[0] for value in (joined_shard, output_shard, entries[0])
    )
    head = tuple(bits[:-3:-1])
    up_order, down_order = tuple(middle) + (core,), tuple(middle[::-1]) + (core,)
    gathered = gather_rows(
        [joined_shard, entries[0], output_shard] + entries[1:],
        (
            (0, 0, rows // 2, head + up_order),
            (0, rows // 2, rows // 2, head + down_order),
            (1, 0, entry_rows, head + up_order),
            (2, 0, output_rows // 2, head + down_order),
            (2, output_rows // 2, output_rows // 2, head + up_order),
            (3, 0, entry_rows, head + down_order),
            (4, 0, entry_rows, head + up_order),
            (5, 0, entry_rows, head + down_order),
            (6, 0, entry_rows, head + up_order),
        ),
        1,
        (devices,) * 7,
        feed_first,
        tuple(distant),
    )
    full_joined, full_f_entry, full_output, full_o_entry = gathered[:4]
    full_g_entry, full_u_entry, full_d_exit, *first_moved = gathered[4:]

    def spread(piece, moved):
        pieces = [piece]
        for bit, came in zip(distant, moved, strict=True):
            pieces.append(came)
            for held in pieces[1:-1]:
                pieces.append(swapped(held, bit))
        return pieces

    full_joined, *first_moved = lax.optimization_barrier((full_joined, *first_moved))
    first_pieces = spread(feed_first, first_moved)

    members = 1 << 3
    place = me % members
    blocks = (me - place) * number
    index = blocks + lax.iota(jnp.int32, members * number)
    all_sequence, all_position, all_chosen = sequence_info(lengths, adapter_set, index)
    all_select = adapter_mask(all_chosen, columns)
    mine = lambda value: lax.dynamic_slice_in_dim(value, place * number, number, 0)
    select = mine(all_select)
    cosine, sine = rotary_tables(mine(all_position))
    key_index = first - REACH * number + lax.iota(jnp.int32, (REACH + 1) * number)
    key_sequence, _, _ = sequence_info(lengths, adapter_set, key_index)
    query_seq = mine(all_sequence)[:, None]
    key_seq = key_sequence[None, :]

    inputs = tokens.astype(jnp.float32)
    gain_one = attention_gain.astype(jnp.float32)
    gain_two = feedforward_gain.astype(jnp.float32)

    down_back = masked(ADAPTER_SCALE * product(cotangent, full_d_exit), select)
    wide_cot = jnp.concatenate([cotangent, down_back], axis=1)
    cot_side = swapped(wide_cot, side)
    cot_line = swapped(wide_cot, line)

    normed_one, unit_one, scale_one = norm_forward(inputs, gain_one)
    normed_one = normed_one.astype(jnp.bfloat16)
    joined_low = masked(product(normed_one, full_f_entry), select)
    half_low = joined_low * ADAPTER_SCALE
    query, pair = joined_heads(
        jnp.concatenate([normed_one, half_low], axis=1), full_joined, cosine, sine
    )
    context = context_of(pair, 4)
    context, feed_second = lax.optimization_barrier((context, feed_second))
    second_moved = []
    for bit in distant[1:]:
        second_moved.append(swapped(feed_second, bit))
    attended = attend(query, context, pair, query_seq, key_seq)
    output_low = masked(product(attended, full_o_entry), select)
    branch = project(
        jnp.concatenate([attended, output_low * ADAPTER_SCALE], axis=1), full_output
    )
    hidden_one = inputs + branch

    normed_two, unit_two, scale_two = norm_forward(hidden_one, gain_two)
    normed_two = normed_two.astype(jnp.bfloat16)
    normed_two, second = lax.optimization_barrier((normed_two, feed_second))
    second_moved = [swapped(second, distant[0])] + second_moved
    second_pieces = spread(feed_second, second_moved)
    half_rows = number // 2
    up_group, down_group = (side, line, core), (line, side, core)
    group_normed, group_cot = gather_rows(
        [normed_two],
        ((0, 0, half_rows, up_group), (0, half_rows, half_rows, down_group)),
        5,
        (members,),
        shared=(
            (0, wide_cot, None),
            (side, cot_side, (0, half_rows, line)),
            (line, cot_line, (half_rows, half_rows, side)),
        ),
    )
    gate_low = masked(product(group_normed, full_g_entry), all_select) * ADAPTER_SCALE
    up_low = masked(product(group_normed, full_u_entry), all_select) * ADAPTER_SCALE
    feeding = (group_normed, group_cot, gate_low, up_low)
    *begun, first_grads = feed(*feeding, first_pieces)
    mixed_parts, back_parts, second_grads = feed(*feeding, second_pieces, begun)
    up_sum, down_sum = (core, side, line), (core, line, side)
    (back_sum,) = reduce_rows([back_parts], [((0, members), (up_sum, down_sum) * 2)], 6)
    gate_low_back = masked(ADAPTER_SCALE * back_sum[:, width : width + columns], select)
    up_low_back = masked(ADAPTER_SCALE * back_sum[:, width + columns :], select)
    normed_two_back = (
        back_sum[:, :width]
        + project(gate_low_back, full_g_entry)
        + project(up_low_back, full_u_entry)
    )
    hidden_back_one = cotangent.astype(jnp.float32) + norm_backward(
        normed_two_back, unit_two, scale_two, gain_two
    )
    branch_back = hidden_back_one.astype(jnp.bfloat16)

    through = product(branch_back, full_output)
    output_low_back = masked(ADAPTER_SCALE * through[:, width:], select)
    attended_back = (through[:, :width] + project(output_low_back, full_o_entry)).astype(
        jnp.bfloat16
    )
    query_back, own_back, away = attend_back(
        query, attended_back, context, pair, query_seq, key_seq, cosine, sine
    )
    orders = ((core,) + tuple(middle) + head[::-1], (core,) + tuple(middle[::-1]) + head[::-1])
    places = tuple((mask, at) for at, mask in enumerate(span(distant)))
    pair_back, mixed_sum, *early = context_back(
        away,
        own_back,
        [
            mixed_parts,
            first_grads,
            second_grads,
            contract_rows(attended, output_low_back),
            ADAPTER_SCALE * contract_rows(branch_back, output_low),
            contract_rows(normed_two, gate_low_back),
            contract_rows(normed_two, up_low_back),
        ],
        [((0, members), (up_sum, down_sum))]
        + [((at, places), (tuple(distant[::-1]),)) for at in (1, 2)]
        + [((at, devices), orders) for at in (3, 4, 5, 6)],
        7,
    )
    down_low = masked(mixed_sum[:, width:], select)
    mixed = mixed_sum[:, :width] + ADAPTER_SCALE * project(down_low, full_d_exit)
    layer_output = (hidden_one + mixed).astype(jnp.bfloat16)

    half = HEAD_WIDTH // 2
    key_back = pair_back[0].reshape(number, KV_HEADS, HEAD_WIDTH)
    rolled = jnp.concatenate([key_back[..., half:], key_back[..., :half]], axis=-1)
    key_back = key_back * cosine[:, None, :] - rolled * sine[:, None, :]
    joined_back = jnp.concatenate(
        [
            query_back,
            key_back.reshape(number, kv_width).astype(jnp.bfloat16),
            pair_back[1].astype(jnp.bfloat16),
        ],
        axis=1,
    )
    inward = product(joined_back, full_joined)
    joined_low_back = masked(ADAPTER_SCALE * inward[:, width:], select)
    normed_one_back = inward[:, :width] + project(joined_low_back, full_f_entry)
    grad_tokens = hidden_back_one + norm_backward(normed_one_back, unit_one, scale_one, gain_one)

    totals = [
        ADAPTER_SCALE * contract_rows(cotangent, down_low),
        contract_rows(joined_back, half_low),
        contract_rows(normed_one, joined_low_back),
    ]
    d_exit, f_exit, f_entry = reduce_rows(
        totals, [((at, devices), orders) for at in range(len(totals))], 8
    )
    feed_rows = jnp.concatenate(early[:2], axis=0)
    o_entry, o_exit, g_entry, u_entry = early[2:]
    return (
        layer_output,
        grad_tokens,
        f_entry,
        f_exit,
        o_entry,
        o_exit,
        g_entry,
        feed_rows[:, :columns],
        u_entry,
        feed_rows[:, columns : 2 * columns],
        feed_rows[:, 2 * columns :],
        d_exit,
    )


def solution(mesh):
    split, copied = P(AXIS, None), P()
    placed = (split, copied, copied) + (split,) * 15 + (copied, copied, split)
    return jax.shard_map(
        layer, mesh=mesh, in_specs=placed, out_specs=(split,) * 12, check_vma=False
    )
```

```python
import functools
import math

import jax
import jax.numpy as jnp
from jax import lax
from jax.experimental import pallas as pl
from jax.experimental.pallas import tpu as pltpu
from jax.sharding import PartitionSpec as P


HEADS = 16
KV_HEADS = 8
HEAD_WIDTH = 128
ADAPTER_RANK = 16
REACH = 4

EPSILON = 1e-05
ADAPTER_SCALE = 0.5
ROTARY_BASE = 1000000.0
MASKED = -1e30
MESH = pl.DeviceIdType.MESH
AXIS = "fsdp"
VMEM_LIMIT = 60 * 1024 * 1024


def swapped(value, bit):
    count = lax.axis_size(AXIS)
    return lax.ppermute(value, AXIS, [(source, source ^ bit) for source in range(count)])


def project(left, right):
    return lax.dot_general(
        left, right, (((1,), (1,)), ((), ())), preferred_element_type=jnp.float32
    )


def product(left, right):
    return jnp.dot(left, right, preferred_element_type=jnp.float32)


def contract_rows(left, right):
    return lax.dot_general(
        left, right, (((0,), (0,)), ((), ())), preferred_element_type=jnp.float32
    )


def sequence_info(lengths, adapter_set, index):
    ends = jnp.cumsum(lengths)
    starts = ends - lengths
    member = (index[:, None] >= starts[None, :]) & (index[:, None] < ends[None, :])
    labels = lax.iota(jnp.int32, lengths.shape[0]) + 1
    sequence = jnp.sum(jnp.where(member, labels[None, :], 0), axis=1) - 1
    begin = jnp.sum(jnp.where(member, starts[None, :], 0), axis=1)
    chosen = jnp.sum(jnp.where(member, adapter_set[None, :], 0), axis=1)
    return (sequence, index - begin, chosen)


def adapter_mask(chosen, columns):
    column_set = lax.broadcasted_iota(jnp.int32, (1, columns), 1) // ADAPTER_RANK
    return column_set == chosen[:, None]


def masked(values, select):
    return jnp.where(select, values, 0.0).astype(jnp.bfloat16)


def rotary_tables(position):
    half = HEAD_WIDTH // 2
    inverse = jnp.exp(lax.iota(jnp.float32, half) * (-2.0 * math.log(ROTARY_BASE) / HEAD_WIDTH))
    angles = position.astype(jnp.float32)[:, None] * inverse[None, :]
    cosine, sine = jnp.cos(angles), jnp.sin(angles)
    return (
        jnp.concatenate([cosine, cosine], axis=1),
        jnp.concatenate([-sine, sine], axis=1),
    )


def norm_forward(values, gain):
    scale = lax.rsqrt(jnp.mean(values * values, axis=-1, keepdims=True) + EPSILON)
    unit = values * scale
    return (unit * gain, unit, scale)


def norm_backward(grad, unit, scale, gain):
    weighted = grad * gain
    return scale * (weighted - unit * jnp.mean(weighted * unit, axis=-1, keepdims=True))


def partner_of(me, bit):
    return me + bit - 2 * bit * ((me // bit) % 2)


def peer_of(me, mask):
    bit = 1
    while bit <= mask:
        if mask & bit:
            me = partner_of(me, bit)
        bit *= 2
    return me


def enter(me, bits):
    barrier = pltpu.get_barrier_semaphore()
    for bit in bits:
        pl.semaphore_signal(
            barrier, inc=1, device_id=(partner_of(me, bit),), device_id_type=MESH
        )
    pl.semaphore_wait(barrier, len(bits))


def span(bits):
    held = [0]
    for bit in bits:
        held = held + [mask + bit for mask in held]
    return held


def gather_kernel(parts, slots, bits_moved, shared, count, *refs):
    extra = len(shared) or (len(bits_moved) > 0)
    added = 1 if shared else len(bits_moved)
    ins, more = refs[:count], refs[count : count + extra]
    outs = refs[count + extra : 2 * count + extra]
    away = refs[2 * count + extra : 2 * count + extra + added]
    send, recv, local, *stage = refs[2 * count + extra + added :]
    me = lax.axis_index(AXIS)
    enter(me, sorted({bit for part in parts for bit in part[3]}))

    def block(p, mask):
        a, first, number, _ = parts[p]
        rows = ins[a].shape[0]
        start = pl.multiple_of(peer_of(me, mask) % slots[a] * rows + first, 8)
        return outs[a].at[pl.ds(start, number)]

    def own(p):
        a, first, number, _ = parts[p]
        return ins[a].at[pl.ds(first, number)]

    def copy(p, mask, bit):
        return pltpu.make_async_remote_copy(
            src_ref=own(p) if mask == 0 else block(p, mask),
            dst_ref=block(p, mask),
            send_sem=send.at[p, mask + bit],
            recv_sem=recv.at[p, mask + bit],
            device_id=(partner_of(me, bit),),
            device_id_type=MESH,
        )

    def arrive(p, mask, bit):
        pltpu.make_async_remote_copy(
            src_ref=block(p, mask),
            dst_ref=block(p, mask),
            send_sem=send.at[p, mask],
            recv_sem=recv.at[p, mask],
            device_id=(partner_of(me, bit),),
            device_id_type=MESH,
        ).wait_recv()

    sends, arrivals = [], []
    for p, (_, _, _, order) in enumerate(parts):
        for level, bit in enumerate(order):
            first = copy(p, 0, bit)
            first.start()
            sends.append(first)
            for place, mask in enumerate(span(order[:level])):
                arrivals.append(((level, place, p), p, mask + bit, bit, order[level + 1 :]))
    kept, exchanged = [], []

    def keep(at, source, target):
        inward = pltpu.make_async_copy(source, stage[at], local.at[0, at])
        inward.start()
        kept.append((inward, pltpu.make_async_copy(stage[at], target, local.at[1, at])))

    def there(mask, first, rows):
        height = away[0].shape[0] // slots[-1]
        start = pl.multiple_of(peer_of(me, mask) % slots[-1] * height + first, 8)
        return away[0].at[pl.ds(start, rows)]

    def hand(at, source, target, bit):
        return pltpu.make_async_remote_copy(
            src_ref=source,
            dst_ref=target,
            send_sem=send.at[len(parts), at],
            recv_sem=recv.at[len(parts), at],
            device_id=(partner_of(me, bit),),
            device_id_type=MESH,
        )

    crossed = []
    for i, (mask, crossing) in enumerate(shared):
        if crossing is not None:
            first, rows, bit = crossing
            crossed.append(
                hand(8 + i, more[i].at[pl.ds(first, rows)], there(mask, first, rows), bit)
            )
            crossed[-1].start()
    for i, (mask, _) in enumerate(shared):
        rows = more[i].shape[0]
        exchanged.append(hand(i, more[i], there(mask, 0, rows), 1))
        exchanged[-1].start()
        keep(len(parts) + i, more[i], there(mask, 0, rows))
    for p in range(len(parts)):
        keep(p, own(p), block(p, 0))
    for inward, outward in kept:
        inward.wait()
        outward.start()
    arrivals.sort(key=lambda entry: entry[0])
    moves = [
        pltpu.make_async_remote_copy(
            src_ref=more[0],
            dst_ref=away[i],
            send_sem=send.at[len(parts), i],
            recv_sem=recv.at[len(parts), i],
            device_id=(partner_of(me, bit),),
            device_id_type=MESH,
        )
        for i, bit in enumerate(bits_moved)
    ]
    waiting = len(moves) > 0
    for (level, _, _), p, mask, bit, later in arrivals:
        if waiting and level == 1:
            waiting = False
            for move in moves:
                move.start()
        arrive(p, mask, bit)
        for following in later:
            onward = copy(p, mask, following)
            onward.start()
            sends.append(onward)
    crossings = [entry for entry in enumerate(shared) if entry[1][1] is not None]
    for (i, (mask, (first, rows, bit))), sent in zip(crossings, crossed, strict=True):
        came = there(mask + bit, first, rows)
        sent.wait_recv()
        exchanged.append(hand(16 + i, came, came, 1))
        exchanged[-1].start()
    for move in moves + exchanged:
        move.wait()
    for sent in crossed:
        sent.wait_send()
    for sent in sends:
        sent.wait_send()
    for _, outward in kept:
        outward.wait()


def gather_rows(arrays, parts, collective_id, slots, moved=None, bits_moved=(), shared=()):
    count, devices = len(arrays), lax.axis_size(AXIS)
    shapes = [
        jax.ShapeDtypeStruct((times * a.shape[0], a.shape[1]), a.dtype)
        for a, times in zip(arrays, slots)
    ]
    sent = 2 * sum(math.prod(shape.shape) for shape in shapes)
    if moved is not None:
        arrays = list(arrays) + [moved]
        shapes += [jax.ShapeDtypeStruct(moved.shape, moved.dtype)] * len(bits_moved)
    if shared:
        whole = shared[0][1]
        arrays = list(arrays) + [value for _, value, _ in shared]
        shape = (slots[-1] * whole.shape[0], whole.shape[1])
        shapes.append(jax.ShapeDtypeStruct(shape, whole.dtype))
    places = tuple((mask, crossing) for mask, _, crossing in shared)
    return pl.pallas_call(
        functools.partial(gather_kernel, parts, slots, bits_moved, places, count),
        out_shape=shapes,
        in_specs=[pl.BlockSpec(memory_space=pl.ANY)] * len(arrays),
        out_specs=[pl.BlockSpec(memory_space=pl.ANY)] * len(shapes),
        scratch_shapes=[
            pltpu.SemaphoreType.DMA((len(parts) + 1, devices)),
            pltpu.SemaphoreType.DMA((len(parts) + 1, devices)),
            pltpu.SemaphoreType.DMA((2, len(parts) + len(shared))),
        ]
        + [pltpu.VMEM((part[2], arrays[part[0]].shape[1]), arrays[part[0]].dtype) for part in parts]
        + [pltpu.VMEM(value.shape, value.dtype) for _, value, _ in shared],
        compiler_params=pltpu.CompilerParams(
            collective_id=collective_id, has_side_effects=True
        ),
        cost_estimate=pl.CostEstimate(flops=0, bytes_accessed=8 * sent, transcendentals=0),
        name="gather_rows",
    )(*arrays)


class Halving:
    def __init__(self, me, parts, ins, outs, totals, outgoing, incoming, send, recv):
        self.me, self.parts, self.ins, self.outs = me, parts, ins, outs
        self.totals, self.outgoing, self.incoming = totals, outgoing, incoming
        self.send, self.recv = send, recv
        self.pending = [[] for _ in parts]
        self.every = []
        self.levels = max(len(part[4]) for part in parts)

    def given(self, p, mask):
        _, block, first, rows, _, places, base, _ = self.parts[p]
        a, place = places
        if isinstance(place, int):
            at = peer_of(self.me, mask + base) % place
        else:
            at = dict(place)[mask]
        return self.ins[a].at[pl.ds(pl.multiple_of(at * block + first, 8), rows)]

    def masks(self, p):
        return span(self.parts[p][4][:0:-1])

    def launch(self, p, level):
        order = self.parts[p][4]
        bit, half = order[level], 1 << (len(order) - 1 - level)
        region, copies = pl.ds(half - 1, half), []
        if level:
            self.outgoing[p][region] = self.totals[p][half : 2 * half].astype(jnp.bfloat16)
            copies.append((self.outgoing[p].at[region], region, half))
        else:
            for at, mask in enumerate(self.masks(p)):
                source = self.given(p, mask + bit)
                if source.dtype == jnp.bfloat16:
                    copies.append((source, half - 1 + at, half + at))
                else:
                    self.outgoing[p][half - 1 + at] = source[...].astype(jnp.bfloat16)
            if not copies:
                copies.append((self.outgoing[p].at[region], region, half))
        for source, there, at in copies:
            copy = pltpu.make_async_remote_copy(
                src_ref=source,
                dst_ref=self.incoming[p].at[there],
                send_sem=self.send.at[p, at],
                recv_sem=self.recv.at[p, at],
                device_id=(partner_of(self.me, bit),),
                device_id_type=MESH,
            )
            copy.start()
            self.pending[p].append(copy)
            self.every.append(copy)

    def begin(self):
        for p in range(len(self.parts)):
            self.launch(p, 0)

    def advance(self, level):
        for p, (a, _, _, rows, order, _, _, row) in enumerate(self.parts):
            if level >= len(order):
                continue
            half, wide = 1 << (len(order) - 1 - level), jnp.float32
            arrived, self.pending[p] = self.pending[p], []
            for copy in arrived:
                copy.wait_recv()
            last = level + 1 == len(order)
            if last:
                held = self.totals[p][0] if level else self.given(p, 0)[...].astype(wide)
                total = held + self.incoming[p][0].astype(wide)
                self.outs[a][row : row + rows, :] = total.astype(self.outs[a].dtype)
            elif level:
                came = self.incoming[p][half - 1 : 2 * half - 1].astype(wide)
                self.totals[p][:half] = self.totals[p][:half] + came
            else:
                for at, mask in enumerate(self.masks(p)):
                    came = self.incoming[p][half - 1 + at].astype(wide)
                    self.totals[p][at] = self.given(p, mask)[...].astype(wide) + came
            if not last:
                self.launch(p, level + 1)

    def finish(self):
        for copy in self.every:
            copy.wait_send()


def reduce_kernel(parts, counts, *refs):
    inputs, outputs = counts
    number = len(parts)
    ins, outs = refs[:inputs], refs[inputs : inputs + outputs]
    rest = refs[inputs + outputs :]
    buffers = (rest[i * number : (i + 1) * number] for i in range(3))
    me = lax.axis_index(AXIS)
    enter(me, sorted({bit for part in parts for bit in part[4]}))
    halving = Halving(me, parts, ins, outs, *buffers, *rest[3 * number :])
    halving.begin()
    for level in range(halving.levels):
        halving.advance(level)
    halving.finish()


def reduce_plan(values, sums, steps=()):
    parts, shapes, scratch = [], [], []

    def add(part, columns, given):
        members, rows = 1 << len(part[4]), part[3]
        held = members // 2 if given == jnp.bfloat16 else members
        sizes = (members // 2 if members > 2 else 0, held - 1, members - 1)
        parts.append(part)
        scratch.append([(n, rows, columns) if n else (1, 8, 128) for n in sizes])

    for a, (places, orders) in enumerate(sums):
        value = values[places[0]]
        block, columns = value.shape[0] >> len(orders[0]), value.shape[1]
        shapes.append(jax.ShapeDtypeStruct((block, columns), jnp.float32))
        pieces = len(orders) if block % (64 * len(orders)) == 0 else 1
        rows = block // pieces
        for i in range(pieces):
            order = orders[(a + i) % len(orders)]
            add((a, block, i * rows, rows, order, places, 0, i * rows), columns, value.dtype)
    for places, bit, members, first, rows, bases, kind in steps:
        value = values[places[0]]
        block, columns = value.shape[0] // members, value.shape[1]
        for i, base in enumerate(bases):
            part = (len(shapes), block, first, rows, (bit,), places, base, i * rows)
            add(part, columns, value.dtype)
        shapes.append(jax.ShapeDtypeStruct((len(bases) * rows, columns), kind))
    most = max(1 << len(part[4]) for part in parts)
    kinds = (jnp.float32, jnp.bfloat16, jnp.bfloat16)
    buffers = [pltpu.VMEM(s[i], kinds[i]) for i in range(3) for s in scratch]
    buffers += [pltpu.SemaphoreType.DMA((len(parts), most))] * 2
    return tuple(parts), shapes, buffers


def reduce_rows(values, sums, collective_id, steps=()):
    parts, shapes, buffers = reduce_plan(values, sums, steps)
    sent = 2 * sum(value.size for value in values)
    return pl.pallas_call(
        functools.partial(reduce_kernel, parts, (len(values), len(shapes))),
        out_shape=shapes,
        in_specs=[pl.BlockSpec(memory_space=pltpu.VMEM)] * len(values),
        out_specs=[pl.BlockSpec(memory_space=pltpu.VMEM)] * len(shapes),
        scratch_shapes=buffers,
        compiler_params=pltpu.CompilerParams(
            collective_id=collective_id, has_side_effects=True, vmem_limit_bytes=67043328
        ),
        cost_estimate=pl.CostEstimate(flops=0, bytes_accessed=16 * sent, transcendentals=0),
        name="reduce_rows",
    )(*values)


def greet(me, devices, steps, bits=(1,)):
    barrier = pltpu.get_barrier_semaphore()
    for bit in bits:
        pl.semaphore_signal(
            barrier, inc=1, device_id=(partner_of(me, bit),), device_id_type=MESH
        )
    for step in steps:
        for there in (me + step, me - step):
            pl.semaphore_signal(
                barrier, inc=1, device_id=((there + devices) % devices,), device_id_type=MESH
            )
    pl.semaphore_wait(barrier, len(bits) + 2 * len(steps))


def context_kernel(devices, pair_ref, out_ref, zero, send, recv, local):
    me = lax.axis_index(AXIS)
    greet(me, devices, (2, 4))
    even = me % 2 == 0
    partner = partner_of(me, 1)

    def copy(i, source, slot, there):
        return pltpu.make_async_remote_copy(
            src_ref=source,
            dst_ref=out_ref.at[slot],
            send_sem=send.at[i],
            recv_sem=recv.at[slot],
            device_id=(there,),
            device_id_type=MESH,
        )

    def arrive(slot):
        copy(0, out_ref.at[slot], slot, partner).wait_recv()

    two = copy(0, pair_ref, 2, (me + 2) % devices)
    four = copy(1, pair_ref, 0, (me + 4) % devices)
    own = copy(2, pair_ref, 3, partner)
    two_even = copy(3, out_ref.at[2], 1, partner)
    two_odd = copy(3, out_ref.at[2], 3, partner)
    four_odd = copy(2, out_ref.at[0], 1, partner)
    has_two, has_four = me >= 2, me >= 4

    @pl.when(me + 2 < devices)
    def _():
        two.start()

    @pl.when(me + 4 < devices)
    def _():
        four.start()

    @pl.when(even)
    def _():
        own.start()

    @pl.when(me < 4)
    def _():
        zero[...] = jnp.zeros_like(zero)
        pltpu.make_async_copy(zero, out_ref.at[0], local.at[0]).start()

    @pl.when(me < 2)
    def _():
        pltpu.make_async_copy(zero, out_ref.at[2], local.at[2]).start()

    lacks_three = me < 3
    lacks_one = me < 1

    @pl.when(lacks_three)
    def _():
        pltpu.make_async_copy(zero, out_ref.at[1], local.at[1]).start()

    @pl.when(lacks_one)
    def _():
        pltpu.make_async_copy(zero, out_ref.at[3], local.at[3]).start()

    @pl.when(has_two)
    def _():
        arrive(2)

    @pl.when(has_two & even)
    def _():
        two_even.start()

    @pl.when(has_two & (me % 2 == 1))
    def _():
        two_odd.start()

    @pl.when(has_four)
    def _():
        arrive(0)

    @pl.when(has_four & (me % 2 == 1))
    def _():
        four_odd.start()

    @pl.when(me >= 1)
    def _():
        arrive(3)

    @pl.when(me >= 3)
    def _():
        arrive(1)

    for lacks, slot in ((me < 4, 0), (me < 3, 1), (me < 2, 2), (me < 1, 3)):

        @pl.when(lacks)
        def _(slot=slot):
            pltpu.make_async_copy(zero, out_ref.at[slot], local.at[slot]).wait()

    @pl.when(me + 2 < devices)
    def _():
        two.wait_send()

    @pl.when(me + 4 < devices)
    def _():
        four.wait_send()

    @pl.when(even)
    def _():
        own.wait_send()

    @pl.when(has_two)
    def _():
        two_even.wait_send()

    @pl.when(has_four & (me % 2 == 1))
    def _():
        four_odd.wait_send()


def context_of(pair, collective_id):
    devices = lax.axis_size(AXIS)
    return pl.pallas_call(
        functools.partial(context_kernel, devices),
        out_shape=jax.ShapeDtypeStruct((REACH,) + pair.shape, pair.dtype),
        in_specs=[pl.BlockSpec(memory_space=pl.ANY)],
        out_specs=pl.BlockSpec(memory_space=pl.ANY),
        scratch_shapes=[
            pltpu.VMEM(pair.shape, pair.dtype),
            pltpu.SemaphoreType.DMA((REACH,)),
            pltpu.SemaphoreType.DMA((REACH,)),
            pltpu.SemaphoreType.DMA((REACH,)),
        ],
        compiler_params=pltpu.CompilerParams(
            collective_id=collective_id, has_side_effects=True, vmem_limit_bytes=VMEM_LIMIT
        ),
        cost_estimate=pl.CostEstimate(
            flops=0, bytes_accessed=64 * pair.size, transcendentals=0
        ),
        name="context",
    )(pair)


def context_back_kernel(devices, parts, counts, away, own, *refs):
    inputs, outputs = counts
    values, out_ref = refs[:inputs], refs[inputs]
    sums = refs[inputs + 1 : inputs + 1 + outputs]
    refs = refs[inputs + 1 + outputs :]
    beside, going, coming, send, recv = refs[:5]
    number = len(parts)
    buffers = (refs[5 + i * number : 5 + (i + 1) * number] for i in range(3))
    me = lax.axis_index(AXIS)
    bits = sorted({bit for part in parts for bit in part[4]})
    greet(me, devices, (2, 4), bits)
    halving = Halving(me, parts, values, sums, *buffers, *refs[5 + 3 * number :])
    even = me % 2 == 0
    partner = partner_of(me, 1)
    wide, narrow = jnp.float32, jnp.bfloat16

    def copy(i, c, source, target, there):
        return pltpu.make_async_remote_copy(
            src_ref=source,
            dst_ref=target,
            send_sem=send.at[c, i],
            recv_sem=recv.at[c, i],
            device_id=(there,),
            device_id_type=MESH,
        )

    pieces = own.shape[1] // 2
    chunks = [(h, pl.ds(r * pieces, pieces), 2 * h + r) for h in range(2) for r in range(2)]
    shared = []
    for h, rows, c in chunks:
        for i, slot in enumerate((3, 1)):
            shared.append(copy(i, c, away.at[slot, h, rows], beside.at[i, h, rows], partner))
            shared[-1].start()
    halving.begin()
    out_ref[...] = own[...]
    far = []
    for h, rows, c in chunks:
        for i in range(2):
            shared[2 * c + i].wait_recv()
        one, three = beside[0, h, rows].astype(wide), beside[1, h, rows].astype(wide)
        first = away[2, h, rows].astype(wide) + jnp.where(even, three, one)
        second = away[0, h, rows].astype(wide) + jnp.where(even, 0.0, three)
        going[0, h, rows] = first.astype(narrow)
        going[1, h, rows] = second.astype(narrow)
        out_ref[h, rows] += jnp.where(even, one, 0.0)
        for i, step in enumerate((2, 4)):
            move = copy(
                2 + i, c, going.at[i, h, rows], coming.at[i, h, rows],
                (me - step + devices) % devices,
            )
            far.append((i, h, rows, step, move))

            @pl.when(me >= step)
            def _(move=move):
                move.start()

    for level in range(halving.levels):
        halving.advance(level)
    for i, h, rows, step, move in far:

        @pl.when(me + step < devices)
        def _(i=i, h=h, rows=rows, move=move):
            move.wait_recv()
            out_ref[h, rows] += coming[i, h, rows].astype(wide)

    halving.finish()
    for move in shared:
        move.wait_send()
    for _, _, _, step, move in far:

        @pl.when(me >= step)
        def _(move=move):
            move.wait_send()


def context_back(away, own, values, sums, collective_id):
    devices = lax.axis_size(AXIS)
    half = (2,) + own.shape
    parts, shapes, buffers = reduce_plan(values, sums)
    in_vmem = pl.BlockSpec(memory_space=pltpu.VMEM)
    return pl.pallas_call(
        functools.partial(context_back_kernel, devices, parts, (len(values), len(sums))),
        out_shape=[jax.ShapeDtypeStruct(own.shape, jnp.float32)] + shapes,
        in_specs=[in_vmem] * (2 + len(values)),
        out_specs=[in_vmem] * (1 + len(sums)),
        scratch_shapes=[
            pltpu.VMEM(half, jnp.bfloat16),
            pltpu.VMEM(half, jnp.bfloat16),
            pltpu.VMEM(half, jnp.bfloat16),
            pltpu.SemaphoreType.DMA((4, 4)),
            pltpu.SemaphoreType.DMA((4, 4)),
        ]
        + buffers,
        compiler_params=pltpu.CompilerParams(
            collective_id=collective_id, has_side_effects=True, vmem_limit_bytes=67043328
        ),
        cost_estimate=pl.CostEstimate(flops=0, bytes_accessed=64 * own.size, transcendentals=0),
        name="context_back",
    )(away, own, *values)


def joined_kernel(turned, x_ref, w_ref, cos_ref, sin_ref, query_ref, pair_ref):
    step = pl.program_id(0)
    values = project(x_ref[...], w_ref[...])
    cosine, sine = cos_ref[...], sin_ref[...]
    heads = values.shape[1] // HEAD_WIDTH
    turn = step < turned
    pieces = []
    for h in range(heads):
        head = values[:, h * HEAD_WIDTH : (h + 1) * HEAD_WIDTH]
        rotated = head * cosine + pltpu.roll(head, HEAD_WIDTH // 2, 1) * sine
        pieces.append(jnp.where(turn, rotated, head).astype(jnp.bfloat16))
    result = jnp.concatenate(pieces, axis=1)
    half = pl.num_programs(0) // 2

    @pl.when(step < half)
    def _():
        query_ref[...] = result

    @pl.when(step >= half)
    def _():
        pair_ref[...] = result


def joined_heads(x, weight, cosine, sine):
    number, depth = x.shape
    tile = 1024
    steps = weight.shape[0] // tile
    half = steps // 2
    turned = (HEADS + KV_HEADS) * HEAD_WIDTH // tile
    wide = half * tile
    return pl.pallas_call(
        functools.partial(joined_kernel, turned),
        out_shape=[jax.ShapeDtypeStruct((number, wide), jnp.bfloat16)] * 2,
        grid=(steps,),
        in_specs=[
            pl.BlockSpec((number, depth), lambda j: (0, 0), pipeline_mode=pl.Buffered(1)),
            pl.BlockSpec((tile, depth), lambda j: (j, 0)),
            pl.BlockSpec((number, HEAD_WIDTH), lambda j: (0, 0)),
            pl.BlockSpec((number, HEAD_WIDTH), lambda j: (0, 0)),
        ],
        out_specs=[
            pl.BlockSpec((number, tile), lambda j: (0, jnp.minimum(j, half - 1))),
            pl.BlockSpec((number, tile), lambda j: (0, jnp.maximum(j - half, 0))),
        ],
        compiler_params=pltpu.CompilerParams(vmem_limit_bytes=VMEM_LIMIT),
        cost_estimate=pl.CostEstimate(
            flops=2 * number * depth * weight.shape[0],
            bytes_accessed=2 * weight.size + 4 * x.size,
            transcendentals=0,
        ),
        name="joined_heads",
    )(x, weight, cosine, sine)


def make_bias(query_seq, key_seq, bias_ref):
    number, keys = bias_ref.shape
    row = lax.broadcasted_iota(jnp.int32, (number, keys), 0) + (keys - number)
    column = lax.broadcasted_iota(jnp.int32, (number, keys), 1)
    allowed = (query_seq == key_seq) & (column <= row)
    bias_ref[...] = jnp.where(allowed, 0.0, MASKED)


def softmax_of(query, keys, bias):
    scale = HEAD_WIDTH ** (-0.5)
    scores = jnp.concatenate([project(query, key) for key in keys], axis=1) * scale + bias
    top = jnp.max(scores, axis=-1, keepdims=True)
    weights = jnp.exp(scores - top)
    return weights * (1.0 / jnp.sum(weights, axis=-1, keepdims=True))


def attend_kernel(blocks, *refs):
    q_ref = refs[0]
    k_refs = refs[1 : 1 + blocks]
    v_refs = refs[1 + blocks : 1 + 2 * blocks]
    qs_ref, ks_ref, out_ref, bias_ref = refs[1 + 2 * blocks :]

    @pl.when(pl.program_id(0) == 0)
    def _():
        make_bias(qs_ref[...], ks_ref[...], bias_ref)

    keys = [ref[...] for ref in k_refs]
    number = keys[0].shape[0]
    for g in range(HEADS // KV_HEADS):
        columns = slice(g * HEAD_WIDTH, (g + 1) * HEAD_WIDTH)
        probs = softmax_of(q_ref[:, columns], keys, bias_ref[...]).astype(jnp.bfloat16)
        result = product(probs[:, :number], v_refs[0][...])
        for b in range(1, blocks):
            result += product(probs[:, b * number : (b + 1) * number], v_refs[b][...])
        out_ref[:, columns] = result.astype(jnp.bfloat16)


def context_specs(number, blocks):
    def at(b, shift):
        if b == blocks - 1:
            return pl.BlockSpec((number, HEAD_WIDTH), lambda j: (0, shift + j))
        return pl.BlockSpec((None, number, HEAD_WIDTH), lambda j: (b, 0, shift + j))

    return [at(b, 0) for b in range(blocks)] + [at(b, KV_HEADS) for b in range(blocks)]


def attend(query, context, pair, query_seq, key_seq):
    number, blocks = query.shape[0], context.shape[0] + 1
    pairs = [context] * (blocks - 1) + [pair]
    group = HEADS // KV_HEADS
    keys = blocks * number
    wide_spec = pl.BlockSpec((number, group * HEAD_WIDTH), lambda j: (0, j))
    return pl.pallas_call(
        functools.partial(attend_kernel, blocks),
        out_shape=jax.ShapeDtypeStruct(query.shape, jnp.bfloat16),
        grid=(KV_HEADS,),
        in_specs=[wide_spec]
        + context_specs(number, blocks)
        + [
            pl.BlockSpec((number, 1), lambda j: (0, 0)),
            pl.BlockSpec((1, keys), lambda j: (0, 0)),
        ],
        out_specs=wide_spec,
        scratch_shapes=[pltpu.VMEM((number, keys), jnp.float32)],
        compiler_params=pltpu.CompilerParams(vmem_limit_bytes=VMEM_LIMIT),
        cost_estimate=pl.CostEstimate(
            flops=4 * HEADS * number * keys * HEAD_WIDTH,
            bytes_accessed=4 * query.size + 2 * blocks * pair.size,
            transcendentals=HEADS * number * keys,
        ),
        name="attend",
    )(query, *pairs, *pairs, query_seq, key_seq)


def attend_back_kernel(blocks, *refs):
    q_ref, g_ref = refs[:2]
    k_refs = refs[2 : 2 + blocks]
    v_refs = refs[2 + blocks : 2 + 2 * blocks]
    qs_ref, ks_ref, cos_ref, sin_ref = refs[2 + 2 * blocks : 6 + 2 * blocks]
    dq_ref, own_ref, away_ref, bias_ref = refs[6 + 2 * blocks :]

    @pl.when(pl.program_id(0) == 0)
    def _():
        make_bias(qs_ref[...], ks_ref[...], bias_ref)

    scale = HEAD_WIDTH ** (-0.5)
    keys = [ref[...] for ref in k_refs]
    number = keys[0].shape[0]
    key_back = [None] * blocks
    value_back = [None] * blocks
    for g in range(HEADS // KV_HEADS):
        columns = slice(g * HEAD_WIDTH, (g + 1) * HEAD_WIDTH)
        query, grad = q_ref[:, columns], g_ref[:, columns]
        probs = softmax_of(query, keys, bias_ref[...])
        back = jnp.concatenate([project(grad, ref[...]) for ref in v_refs], axis=1)
        center = jnp.sum(back * probs, axis=-1, keepdims=True)
        score_back = (probs * (back - center)).astype(jnp.bfloat16)
        probs = probs.astype(jnp.bfloat16)
        total = None
        for b in range(blocks):
            rows = slice(b * number, (b + 1) * number)
            part = product(score_back[:, rows], keys[b])
            total = part if total is None else total + part
            to_key = contract_rows(score_back[:, rows], query)
            to_value = contract_rows(probs[:, rows], grad)
            key_back[b] = to_key if g == 0 else key_back[b] + to_key
            value_back[b] = to_value if g == 0 else value_back[b] + to_value
        total = total * scale
        turned = total * cos_ref[...] - pltpu.roll(total, HEAD_WIDTH // 2, 1) * sin_ref[...]
        dq_ref[:, columns] = turned.astype(jnp.bfloat16)
    for b in range(blocks - 1):
        away_ref[b, 0] = (key_back[b] * scale).astype(jnp.bfloat16)
        away_ref[b, 1] = value_back[b].astype(jnp.bfloat16)
    own_ref[0] = key_back[blocks - 1] * scale
    own_ref[1] = value_back[blocks - 1]


def attend_back(query, grad, context, pair, query_seq, key_seq, cosine, sine):
    number, blocks = query.shape[0], context.shape[0] + 1
    pairs = [context] * (blocks - 1) + [pair]
    group = HEADS // KV_HEADS
    keys = blocks * number
    wide = KV_HEADS * HEAD_WIDTH
    wide_spec = pl.BlockSpec((number, group * HEAD_WIDTH), lambda j: (0, j))
    fixed = pl.BlockSpec((number, HEAD_WIDTH), lambda j: (0, 0))
    return pl.pallas_call(
        functools.partial(attend_back_kernel, blocks),
        out_shape=[
            jax.ShapeDtypeStruct(query.shape, jnp.bfloat16),
            jax.ShapeDtypeStruct((2, number, wide), jnp.float32),
            jax.ShapeDtypeStruct((blocks - 1, 2, number, wide), jnp.bfloat16),
        ],
        grid=(KV_HEADS,),
        in_specs=[wide_spec, wide_spec]
        + context_specs(number, blocks)
        + [
            pl.BlockSpec((number, 1), lambda j: (0, 0)),
            pl.BlockSpec((1, keys), lambda j: (0, 0)),
            fixed,
            fixed,
        ],
        out_specs=[
            wide_spec,
            pl.BlockSpec((2, number, HEAD_WIDTH), lambda j: (0, 0, j)),
            pl.BlockSpec((blocks - 1, 2, number, HEAD_WIDTH), lambda j: (0, 0, 0, j)),
        ],
        scratch_shapes=[pltpu.VMEM((number, keys), jnp.float32)],
        compiler_params=pltpu.CompilerParams(vmem_limit_bytes=VMEM_LIMIT),
        cost_estimate=pl.CostEstimate(
            flops=10 * HEADS * number * keys * HEAD_WIDTH,
            bytes_accessed=6 * query.size + 8 * blocks * pair.size,
            transcendentals=HEADS * number * keys,
        ),
        name="attend_back",
    )(query, grad, *pairs, *pairs, query_seq, key_seq, cosine, sine)


def feed_kernel(pieces, joint, carried, *refs):
    x_ref, c_ref, gl_ref, ul_ref = refs[:4]
    w_refs, begun = refs[4 : 4 + pieces], refs[4 + pieces : 4 + pieces + carried]
    outs = refs[4 + pieces + carried :]
    mixed_ref, back_ref, grads_ref, weights, mixed_acc, back_acc, arrival = outs
    step = pl.program_id(0)
    width, columns = x_ref.shape[1], gl_ref.shape[1]
    rounds, hid = weights.shape[0], weights.shape[1] // 3
    height = hid // joint
    main, side = slice(0, width), slice(width, width + columns)

    def load(i, at, place):
        return [
            pltpu.make_async_copy(
                w_refs[i].at[pl.ds(j * height, height)],
                weights.at[at, pl.ds(j * hid + place * height, height)],
                arrival.at[at, place, j],
            )
            for j in range(3)
        ]

    @pl.when(step == 0)
    def _():
        for i in range(pieces):
            for copy in load(i, i // joint, i % joint):
                copy.start()
        grads_ref[...] = jnp.zeros_like(grads_ref)

    for acc, start in zip((mixed_acc, back_acc), begun or (None, None), strict=True):
        acc[...] = jnp.zeros_like(acc) if start is None else start[...].astype(jnp.float32)

    @pl.loop(0, rounds)
    def _(i):
        @pl.when(step == 0)
        def _():
            for place in range(joint):
                for copy in load(0, i, place):
                    copy.wait()

        wg, wu, wd = (weights.at[i, pl.ds(j * hid, hid)] for j in range(3))
        x, gl, ul = x_ref[...], gl_ref[...], ul_ref[...]
        gate = project(x, wg[:, main]) + project(gl, wg[:, side])
        up = project(x, wu[:, main]) + project(ul, wu[:, side])
        back = project(c_ref[...], wd[...])
        sigma = 1.0 / (1.0 + jnp.exp(-gate))
        active = gate * sigma
        hidden = (active * up).astype(jnp.bfloat16)
        gate_back = (back * up * sigma * (1.0 + gate * (1.0 - sigma))).astype(jnp.bfloat16)
        up_back = (back * active).astype(jnp.bfloat16)
        mixed_acc[...] += product(hidden, wd[...])
        back_acc[:, main] += product(gate_back, wg[:, main]) + product(up_back, wu[:, main])
        back_acc[:, side] += product(gate_back, wg[:, side])
        back_acc[:, width + columns :] += product(up_back, wu[:, side])
        at = pl.ds(pl.multiple_of(i * hid, hid), hid)
        grads_ref[at, :columns] += contract_rows(gate_back, gl)
        grads_ref[at, columns : 2 * columns] += contract_rows(up_back, ul)
        grads_ref[at, 2 * columns :] += contract_rows(hidden, c_ref[:, side])

    mixed_ref[...] = mixed_acc[...].astype(jnp.bfloat16)
    back_ref[...] = back_acc[...].astype(jnp.bfloat16)


def feed(x, cot, gate_low, up_low, weights, begun=()):
    (rows, width), columns = x.shape, gate_low.shape[1]
    pieces, height = len(weights), weights[0].shape[0] // 3
    hidden, tile = pieces * height, 256
    hid = min(512, hidden)
    row = lambda wide: pl.BlockSpec((tile, wide), lambda i: (i, 0))
    size = sum(w.size for w in weights)
    return pl.pallas_call(
        functools.partial(feed_kernel, pieces, hid // height, len(begun)),
        out_shape=[
            jax.ShapeDtypeStruct((rows, width + columns), jnp.bfloat16),
            jax.ShapeDtypeStruct((rows, width + 2 * columns), jnp.bfloat16),
            jax.ShapeDtypeStruct((hidden, 3 * columns), jnp.float32),
        ],
        grid=(rows // tile,),
        in_specs=[row(width), row(width + columns), row(columns), row(columns)]
        + [pl.BlockSpec(memory_space=pl.ANY)] * pieces
        + [row(value.shape[1]) for value in begun],
        out_specs=[
            row(width + columns),
            row(width + 2 * columns),
            pl.BlockSpec((hidden, 3 * columns), lambda i: (0, 0)),
        ],
        scratch_shapes=[
            pltpu.VMEM((hidden // hid, 3 * hid, width + columns), jnp.bfloat16),
            pltpu.VMEM((tile, width + columns), jnp.float32),
            pltpu.VMEM((tile, width + 2 * columns), jnp.float32),
            pltpu.SemaphoreType.DMA((hidden // hid, hid // height, 3)),
        ],
        compiler_params=pltpu.CompilerParams(vmem_limit_bytes=VMEM_LIMIT),
        cost_estimate=pl.CostEstimate(
            flops=4 * rows * size,
            bytes_accessed=2 * size + 14 * rows * width,
            transcendentals=rows * hidden,
        ),
        name="feed",
    )(x, cot, gate_low, up_low, *weights, *begun)


def layer(
    tokens,
    attention_gain,
    feedforward_gain,
    joined_projection,
    output_projection,
    gate_weight,
    up_weight,
    down_weight,
    joined_adapter_input,
    joined_adapter_output,
    output_adapter_input,
    output_adapter_output,
    gate_adapter_input,
    gate_adapter_output,
    upward_adapter_input,
    upward_adapter_output,
    down_adapter_input,
    down_adapter_output,
    lengths,
    adapter_set,
    cotangent,
):
    number, width = tokens.shape
    columns = joined_adapter_input.shape[1]
    devices = lax.axis_size(AXIS)
    kv_width = KV_HEADS * HEAD_WIDTH
    bits = [1 << i for i in range(devices.bit_length() - 1)]
    core, side, line = bits[:3]
    distant = bits[:2:-1]
    middle = bits[1:-2]
    me = lax.axis_index(AXIS)
    first = me * number

    joined_shard = jnp.concatenate([joined_projection, joined_adapter_output], axis=1)
    output_shard = jnp.concatenate([output_projection, output_adapter_output], axis=1)
    half_shard = gate_weight.shape[0] // 2

    def feed_half(at):
        pairs = (
            (gate_weight, gate_adapter_output),
            (up_weight, upward_adapter_output),
            (down_weight, down_adapter_input),
        )
        cut = lambda value: value[at * half_shard : (at + 1) * half_shard]
        return jnp.concatenate(
            [jnp.concatenate([cut(left), cut(right)], axis=1) for left, right in pairs], axis=0
        )

    feed_first, feed_second = feed_half(0), feed_half(1)
    entries = [
        joined_adapter_input,
        output_adapter_input,
        gate_adapter_input,
        upward_adapter_input,
        down_adapter_output,
    ]
    rows, output_rows, entry_rows = (
        value.shape[0] for value in (joined_shard, output_shard, entries[0])
    )
    head = tuple(bits[:-3:-1])
    up_order, down_order = tuple(middle) + (core,), tuple(middle[::-1]) + (core,)
    gathered = gather_rows(
        [joined_shard, entries[0], output_shard] + entries[1:],
        (
            (0, 0, rows // 2, head + up_order),
            (0, rows // 2, rows // 2, head + down_order),
            (1, 0, entry_rows, head + up_order),
            (2, 0, output_rows // 2, head + down_order),
            (2, output_rows // 2, output_rows // 2, head + up_order),
            (3, 0, entry_rows, head + down_order),
            (4, 0, entry_rows, head + up_order),
            (5, 0, entry_rows, head + down_order),
            (6, 0, entry_rows, head + up_order),
        ),
        1,
        (devices,) * 7,
        feed_first,
        tuple(distant),
    )
    full_joined, full_f_entry, full_output, full_o_entry = gathered[:4]
    full_g_entry, full_u_entry, full_d_exit, *first_moved = gathered[4:]

    def spread(piece, moved):
        pieces = [piece]
        for bit, came in zip(distant, moved, strict=True):
            pieces.append(came)
            for held in pieces[1:-1]:
                pieces.append(swapped(held, bit))
        return pieces

    full_joined, *first_moved = lax.optimization_barrier((full_joined, *first_moved))
    first_pieces = spread(feed_first, first_moved)

    members = 1 << 3
    place = me % members
    blocks = (me - place) * number
    index = blocks + lax.iota(jnp.int32, members * number)
    all_sequence, all_position, all_chosen = sequence_info(lengths, adapter_set, index)
    all_select = adapter_mask(all_chosen, columns)
    mine = lambda value: lax.dynamic_slice_in_dim(value, place * number, number, 0)
    select = mine(all_select)
    cosine, sine = rotary_tables(mine(all_position))
    key_index = first - REACH * number + lax.iota(jnp.int32, (REACH + 1) * number)
    key_sequence, _, _ = sequence_info(lengths, adapter_set, key_index)
    query_seq = mine(all_sequence)[:, None]
    key_seq = key_sequence[None, :]

    inputs = tokens.astype(jnp.float32)
    gain_one = attention_gain.astype(jnp.float32)
    gain_two = feedforward_gain.astype(jnp.float32)

    down_back = masked(ADAPTER_SCALE * product(cotangent, full_d_exit), select)
    wide_cot = jnp.concatenate([cotangent, down_back], axis=1)
    cot_side = swapped(wide_cot, side)
    cot_line = swapped(wide_cot, line)

    normed_one, unit_one, scale_one = norm_forward(inputs, gain_one)
    normed_one = normed_one.astype(jnp.bfloat16)
    joined_low = masked(product(normed_one, full_f_entry), select)
    half_low = joined_low * ADAPTER_SCALE
    query, pair = joined_heads(
        jnp.concatenate([normed_one, half_low], axis=1), full_joined, cosine, sine
    )
    context = context_of(pair, 4)
    context, feed_second = lax.optimization_barrier((context, feed_second))
    second_moved = []
    for bit in distant[1:]:
        second_moved.append(swapped(feed_second, bit))
    attended = attend(query, context, pair, query_seq, key_seq)
    output_low = masked(product(attended, full_o_entry), select)
    branch = project(
        jnp.concatenate([attended, output_low * ADAPTER_SCALE], axis=1), full_output
    )
    hidden_one = inputs + branch

    normed_two, unit_two, scale_two = norm_forward(hidden_one, gain_two)
    normed_two = normed_two.astype(jnp.bfloat16)
    normed_two, second = lax.optimization_barrier((normed_two, feed_second))
    second_moved = [swapped(second, distant[0])] + second_moved
    second_pieces = spread(feed_second, second_moved)
    half_rows = number // 2
    up_group, down_group = (side, line, core), (line, side, core)
    group_normed, group_cot = gather_rows(
        [normed_two],
        ((0, 0, half_rows, up_group), (0, half_rows, half_rows, down_group)),
        5,
        (members,),
        shared=(
            (0, wide_cot, None),
            (side, cot_side, (0, half_rows, line)),
            (line, cot_line, (half_rows, half_rows, side)),
        ),
    )
    gate_low = masked(product(group_normed, full_g_entry), all_select) * ADAPTER_SCALE
    up_low = masked(product(group_normed, full_u_entry), all_select) * ADAPTER_SCALE
    feeding = (group_normed, group_cot, gate_low, up_low)
    *begun, first_grads = feed(*feeding, first_pieces)
    mixed_parts, back_parts, second_grads = feed(*feeding, second_pieces, begun)
    up_sum, down_sum = (core, side, line), (core, line, side)
    step = lambda first, bases, kind: (
        (1, members), core, members, first, half_rows, bases, kind
    )
    back_sum, keep_up, send_up, keep_down, send_down = reduce_rows(
        [back_parts, mixed_parts],
        [((0, members), (up_sum, down_sum) * 2)],
        6,
        (
            step(0, (0, line), jnp.float32),
            step(0, (side, side + line), jnp.bfloat16),
            step(half_rows, (0, side), jnp.float32),
            step(half_rows, (line, side + line), jnp.bfloat16),
        ),
    )
    came_up = swapped(send_up, side)
    came_down = swapped(send_down, line)
    gate_low_back = masked(ADAPTER_SCALE * back_sum[:, width : width + columns], select)
    up_low_back = masked(ADAPTER_SCALE * back_sum[:, width + columns :], select)
    normed_two_back = (
        back_sum[:, :width]
        + project(gate_low_back, full_g_entry)
        + project(up_low_back, full_u_entry)
    )
    hidden_back_one = cotangent.astype(jnp.float32) + norm_backward(
        normed_two_back, unit_two, scale_two, gain_two
    )
    branch_back = hidden_back_one.astype(jnp.bfloat16)

    through = product(branch_back, full_output)
    output_low_back = masked(ADAPTER_SCALE * through[:, width:], select)
    attended_back = (through[:, :width] + project(output_low_back, full_o_entry)).astype(
        jnp.bfloat16
    )
    query_back, own_back, away = attend_back(
        query, attended_back, context, pair, query_seq, key_seq, cosine, sine
    )
    orders = ((core,) + tuple(middle) + head[::-1], (core,) + tuple(middle[::-1]) + head[::-1])
    places = tuple((mask, at) for at, mask in enumerate(span(distant)))
    mixed_up = keep_up + came_up.astype(jnp.float32)
    mixed_down = keep_down + came_down.astype(jnp.float32)
    pair_back, mixed_up, mixed_down, *early = context_back(
        away,
        own_back,
        [
            mixed_up,
            mixed_down,
            first_grads,
            second_grads,
            contract_rows(attended, output_low_back),
            ADAPTER_SCALE * contract_rows(branch_back, output_low),
            contract_rows(normed_two, gate_low_back),
            contract_rows(normed_two, up_low_back),
        ],
        [((0, ((0, 0), (line, 1))), ((line,),)), ((1, ((0, 0), (side, 1))), ((side,),))]
        + [((at, places), (tuple(distant[::-1]),)) for at in (2, 3)]
        + [((at, devices), orders) for at in (4, 5, 6, 7)],
        7,
    )
    mixed_sum = jnp.concatenate([mixed_up, mixed_down], axis=0)
    down_low = masked(mixed_sum[:, width:], select)
    mixed = mixed_sum[:, :width] + ADAPTER_SCALE * project(down_low, full_d_exit)
    layer_output = (hidden_one + mixed).astype(jnp.bfloat16)

    half = HEAD_WIDTH // 2
    key_back = pair_back[0].reshape(number, KV_HEADS, HEAD_WIDTH)
    rolled = jnp.concatenate([key_back[..., half:], key_back[..., :half]], axis=-1)
    key_back = key_back * cosine[:, None, :] - rolled * sine[:, None, :]
    joined_back = jnp.concatenate(
        [
            query_back,
            key_back.reshape(number, kv_width).astype(jnp.bfloat16),
            pair_back[1].astype(jnp.bfloat16),
        ],
        axis=1,
    )
    inward = product(joined_back, full_joined)
    joined_low_back = masked(ADAPTER_SCALE * inward[:, width:], select)
    normed_one_back = inward[:, :width] + project(joined_low_back, full_f_entry)
    grad_tokens = hidden_back_one + norm_backward(normed_one_back, unit_one, scale_one, gain_one)

    totals = [
        ADAPTER_SCALE * contract_rows(cotangent, down_low),
        contract_rows(joined_back, half_low),
        contract_rows(normed_one, joined_low_back),
    ]
    d_exit, f_exit, f_entry = reduce_rows(
        totals, [((at, devices), orders) for at in range(len(totals))], 8
    )
    feed_rows = jnp.concatenate(early[:2], axis=0)
    o_entry, o_exit, g_entry, u_entry = early[2:]
    return (
        layer_output,
        grad_tokens,
        f_entry,
        f_exit,
        o_entry,
        o_exit,
        g_entry,
        feed_rows[:, :columns],
        u_entry,
        feed_rows[:, columns : 2 * columns],
        feed_rows[:, 2 * columns :],
        d_exit,
    )


def solution(mesh):
    split, copied = P(AXIS, None), P()
    placed = (split, copied, copied) + (split,) * 15 + (copied, copied, split)
    return jax.shard_map(
        layer, mesh=mesh, in_specs=placed, out_specs=(split,) * 12, check_vma=False
    )
```
